256 devices in a mesh: band: 64 (over x, z, y_hi), img: 4 (over y_lo, core).
Axes of the slice: x: 4, y: 4 (y_hi: 2, y_lo: 2; y = y_hi * 2 + y_lo), z: 8, core: 2. Of those that a mesh axis runs over, the one named last changes fastest.
Arguments:
- pixels: bfloat16 [2048, 256, 180], P(('img', 'band')), parts along dimension 0, may hold values from -12 to 12
- keep_mask: int32 [256, 32], P(('img', 'band')), parts along dimension 0, may hold values from 0 to 1, as said below
- band_counts: int32 [256], P(('img', 'band')), parts along dimension 0, may hold values from 0 to 32, as said below
- plan_dest: int32 [256, 16], P(('img', 'band')), parts along dimension 0, may hold values from 0 to 63, as said below
- plan_slot: int32 [256, 16], P(('img', 'band')), parts along dimension 0, may hold values from 0 to 8, as said below
- bias_table: float32 [225, 6], replicated, may hold values from -4 to 4
- gain_attn: float32 [180], replicated, may hold values from 0.25 to 1.75
- qkv_weight: bfloat16 [180, 540], replicated, may hold values from -5 to 5
- proj_weight: bfloat16 [180, 180], replicated, may hold values from -0.4375 to 0.4375
- gain_mlp: float32 [180], replicated, may hold values from 0.25 to 1.75
- hidden_weight: bfloat16 [180, 360], replicated, may hold values from -0.4375 to 0.4375
- output_weight: bfloat16 [360, 180], replicated, may hold values from -0.3125 to 0.3125
Outputs:
- restored: bfloat16 [2048, 256, 180], P(('img', 'band')), parts along dimension 0
- work_tiles: bfloat16 [2048, 128, 180], P(('img', 'band')), parts along dimension 0
The draws below stay inside these ranges and needn't reach their ends.
There are 4 independent parts, one for each index of `img`. The reference program is written for one: setup_inputs(seed, part) draws one part's arguments, and reference() takes and returns one part's arrays. A program takes and returns all parts, laid end to end along the dimension named above; an argument that names none is the same for every part. Nothing has to cross between parts.
Inputs may be any that keep to these rules, and one draw needn't show every extreme that they name: `keep_mask`: the number of ones in a band varies strongly from band to band. band_counts[b] equals the number of ones among band b's windows in keep_mask. A band's live tiles are those with 2 t < band_counts[b]; their number summed over bands lies between 449 and 512, and some band has all 16 tiles live. `plan_dest`: within each aligned group of 64 consecutive tiles of a band (equal t // 64) the destinations are all different. `plan_slot`: 8 for tiles that are not live; a live tile has a slot below 8, no two live tiles of the image share destination and slot, and some destination receives 8 live tiles.
All inputs are finite; a program needn't handle non-finite values.
Results may differ from the reference program's by a relative error of at most 0.0044.
Values may be sent and summed in bfloat16 or wider, within the bound.
No kernel may reach another device: no remote copies, remote signals or barrier semaphores. Data moves between devices by JAX's collectives and lax.ppermute only.
A program may use at most 64 MiB of HBM per device.

```python
import math
import jax
import jax.numpy as jnp
from jax import lax

CHAN = 180
HEADS = 6
FF_WIDTH = 360
WIN = 8
TILE = 2
ROWS = 8
WIDTH = 256
SHIFT = 4
TABLE = 225
HEIGHT = 512
WIN_DEV = 32
TILES_DEV = 16
CAP = 8
N_BAND = 64


def shuffle_band(band_key):
    return jax.random.permutation(band_key, WIN_DEV)


def plan_tables(key):
    key_perm = jax.random.fold_in(key, 101)
    key_share = jax.random.fold_in(key, 102)
    key_cut = jax.random.fold_in(key, 103)
    key_rest = jax.random.fold_in(key, 104)
    key_rank = jax.random.fold_in(key, 105)
    key_turn = jax.random.fold_in(key, 106)
    half_bands = N_BAND // 2
    band_order = jax.random.permutation(key_perm, N_BAND)
    shares = jax.random.randint(key_share, (half_bands,), 1, TILES_DEV + 1).astype(jnp.int32)
    shares = shares.at[0].set(TILES_DEV)
    trimmed = jax.random.randint(key_cut, (), 0, half_bands)
    pair_ids = jnp.arange(half_bands, dtype=jnp.int32)
    lowered = shares - ((pair_ids >= 1) & (pair_ids <= trimmed)).astype(jnp.int32)
    live_tiles = jnp.zeros((N_BAND,), jnp.int32).at[band_order[0::2]].set(lowered).at[band_order[1::2]].set(TILES_DEV - shares)
    spare_windows = jax.random.randint(key_rest, (N_BAND,), 0, TILE).astype(jnp.int32)
    kept_windows = jnp.where(live_tiles > 0, live_tiles * TILE - spare_windows, 0).astype(jnp.int32)
    window_ranks = jax.vmap(shuffle_band)(jax.random.split(key_rank, N_BAND))
    keep_table = (window_ranks < kept_windows[:, None]).astype(jnp.int32).reshape(HEIGHT // WIN, WIDTH // WIN)
    offsets = (jnp.cumsum(live_tiles) - live_tiles).astype(jnp.int32)
    rotation = jax.random.randint(key_turn, (), 0, N_BAND).astype(jnp.int32)
    tile_ids = jnp.arange(TILES_DEV, dtype=jnp.int32)
    global_tile = offsets[:, None] + tile_ids[None, :]
    dest_table = ((global_tile + rotation) % N_BAND).astype(jnp.int32)
    slot_table = jnp.where(tile_ids[None, :] < live_tiles[:, None], global_tile // N_BAND, CAP).astype(jnp.int32)
    return (keep_table, kept_windows, dest_table, slot_table)


def draw_keep_mask(key, part):
    return plan_tables(key)[0]


def draw_band_counts(key, part):
    return plan_tables(key)[1]


def draw_plan_dest(key, part):
    return plan_tables(key)[2]


def draw_plan_slot(key, part):
    return plan_tables(key)[3]


def draw_pixels(key, part):
    base_key = jax.random.fold_in(key, 201)
    values = jnp.clip(jax.random.normal(base_key, (HEIGHT, WIDTH, CHAN), jnp.float32), -6.0, 6.0)
    return values.astype(jnp.bfloat16)


def draw_qkv_weight(key, part):
    main_key = jax.random.fold_in(key, 301)
    weight = jax.random.normal(main_key, (CHAN, 3 * CHAN), jnp.float32) / math.sqrt(CHAN)
    return jnp.clip(weight, -5.0, 5.0).astype(jnp.bfloat16)


def noise(stream_key, shape, width, reach, kind=jnp.bfloat16):
    values = width * jax.random.normal(stream_key, shape, jnp.float32)
    return jnp.clip(values, min=-reach, max=reach).astype(kind)


def setup_inputs(seed: int = 0, part: int = 0) -> dict:
    seeds = jax.random.split(jax.random.key(seed), 13)
    part_keys = jax.random.split(jax.random.fold_in(seeds[12], part), 13)
    return {
        "pixels": draw_pixels(jax.random.fold_in(jax.random.fold_in(seeds[12], part), 71), part),
        "keep_mask": draw_keep_mask(jax.random.fold_in(jax.random.fold_in(seeds[12], part), 71), part),
        "band_counts": draw_band_counts(jax.random.fold_in(jax.random.fold_in(seeds[12], part), 71), part),
        "plan_dest": draw_plan_dest(jax.random.fold_in(jax.random.fold_in(seeds[12], part), 71), part),
        "plan_slot": draw_plan_slot(jax.random.fold_in(jax.random.fold_in(seeds[12], part), 71), part),
        "bias_table": noise(seeds[5], (TABLE, HEADS), 1.0, 4.0, jnp.float32),
        "gain_attn": jnp.clip(1.0 + 0.15 * jax.random.normal(seeds[6], (CHAN,), jnp.float32), 0.25, 1.75),
        "qkv_weight": draw_qkv_weight(jax.random.fold_in(seeds[12], 71), part),
        "proj_weight": noise(seeds[8], (CHAN, CHAN), CHAN ** -0.5, 0.4375),
        "gain_mlp": jnp.clip(1.0 + 0.15 * jax.random.normal(seeds[9], (CHAN,), jnp.float32), 0.25, 1.75),
        "hidden_weight": noise(seeds[10], (CHAN, FF_WIDTH), CHAN ** -0.5, 0.4375),
        "output_weight": noise(seeds[11], (FF_WIDTH, CHAN), FF_WIDTH ** -0.5, 0.3125),
    }


EPSILON = 1e-05

def layer_norm(values, gain_vec):
    values = values.astype(jnp.float32)
    center = values - lax.optimization_barrier(jnp.mean(values, axis=-1, keepdims=True))
    spread = lax.optimization_barrier(jnp.mean(center * center, axis=-1, keepdims=True))
    return center * lax.rsqrt(spread + EPSILON) * gain_vec

def position_bias(bias_table):
    coords = jnp.arange(WIN * WIN, dtype=jnp.int32)
    row_pos = coords // WIN
    col_pos = coords % WIN
    table_index = (row_pos[:, None] - row_pos[None, :] + WIN - 1) * (2 * WIN - 1) + (col_pos[:, None] - col_pos[None, :] + WIN - 1)
    return jnp.transpose(bias_table[table_index], (2, 0, 1))

def region_codes(first_row, row_count, height, col_count):
    rows_global = first_row + jnp.arange(row_count, dtype=jnp.int32)
    row_region = (rows_global >= height - WIN).astype(jnp.int32) + (rows_global >= height - SHIFT).astype(jnp.int32)
    col_global = jnp.arange(col_count, dtype=jnp.int32)
    col_region = (col_global >= col_count - WIN).astype(jnp.int32) + (col_global >= col_count - SHIFT).astype(jnp.int32)
    return 3 * row_region[:, None] + col_region[None, :]

def attend(windows, window_codes, head_bias, gain_attn, qkv_weight, proj_weight):
    window_count = windows.shape[0]
    head_dim = CHAN // HEADS
    normed = layer_norm(windows, gain_attn).astype(jnp.bfloat16).reshape(-1, CHAN)
    mixed_all = jnp.dot(normed, qkv_weight, preferred_element_type=jnp.float32).reshape(window_count, WIN * WIN, 3, HEADS, head_dim)
    queries = mixed_all[:, :, 0] * head_dim ** (-0.5)
    key_part = mixed_all[:, :, 1]
    value_part = lax.optimization_barrier(mixed_all[:, :, 2].astype(jnp.bfloat16)).astype(jnp.float32)
    scores = jnp.einsum('wqhd,wkhd->whqk', queries, key_part, precision=lax.Precision.HIGHEST)
    differ = window_codes[:, :, None] != window_codes[:, None, :]
    scores = scores + head_bias[None] + jnp.where(differ, -100.0, 0.0)[:, None]
    weights = jax.nn.softmax(scores, axis=-1).astype(jnp.bfloat16)
    weights = lax.optimization_barrier(weights).astype(jnp.float32)
    mixed = jnp.einsum('whqk,wkhd->wqhd', weights, value_part, precision=lax.Precision.HIGHEST)
    mixed = mixed.reshape(-1, CHAN).astype(jnp.bfloat16)
    projected = jnp.dot(mixed, proj_weight, preferred_element_type=jnp.float32)
    summed = windows.reshape(-1, CHAN).astype(jnp.float32) + projected
    return summed.astype(jnp.bfloat16).reshape(window_count, WIN * WIN, CHAN)

def feed(states, gain_mlp, hidden_weight, output_weight):
    flat_rows = states.reshape(-1, CHAN)
    normed = layer_norm(flat_rows, gain_mlp).astype(jnp.bfloat16)
    inner_act = jax.nn.gelu(jnp.dot(normed, hidden_weight, preferred_element_type=jnp.float32)).astype(jnp.bfloat16)
    summed = flat_rows.astype(jnp.float32) + jnp.dot(inner_act, output_weight, preferred_element_type=jnp.float32)
    return summed.astype(jnp.bfloat16).reshape(states.shape)

def reference(pixels, keep_mask, band_counts, plan_dest, plan_slot, bias_table, gain_attn, qkv_weight, proj_weight, gain_mlp, hidden_weight, output_weight):
    height = ROWS * N_BAND
    win_rows = ROWS // WIN
    win_cols = WIDTH // WIN
    shifted = jnp.roll(pixels, (-SHIFT, -SHIFT), axis=(0, 1))
    windows = shifted.reshape(N_BAND, win_rows, WIN, win_cols, WIN, CHAN).transpose(0, 1, 3, 2, 4, 5).reshape(N_BAND, WIN_DEV, WIN * WIN, CHAN)
    region_map = region_codes(0, height, height, WIDTH)
    window_codes = region_map.reshape(N_BAND, win_rows, WIN, win_cols, WIN).transpose(0, 1, 3, 2, 4).reshape(N_BAND, WIN_DEV, WIN * WIN)
    keep_rows = keep_mask.reshape(N_BAND, WIN_DEV)
    head_bias = position_bias(bias_table)

    def one_band(band_inputs):
        band_windows, band_codes, band_keep, band_count = band_inputs
        packed_order = (jnp.cumsum(band_keep) - 1).astype(jnp.int32)
        active = (band_keep == 1) & (packed_order < band_count)
        target = jnp.where(active, packed_order, WIN_DEV).astype(jnp.int32)
        packed = jnp.zeros((WIN_DEV + 1, WIN * WIN, CHAN), jnp.bfloat16).at[target].set(band_windows)[:WIN_DEV]
        packed_codes = jnp.zeros((WIN_DEV + 1, WIN * WIN), jnp.int32).at[target].set(band_codes)[:WIN_DEV]
        attended = attend(packed, packed_codes, head_bias, gain_attn, qkv_weight, proj_weight)
        finished = feed(attended, gain_mlp, hidden_weight, output_weight)
        unpacked = finished[jnp.clip(packed_order, 0, WIN_DEV - 1)]
        result = jnp.where(active[:, None, None], unpacked, band_windows)
        return (result, attended.reshape(TILES_DEV, TILE * WIN * WIN, CHAN))
    results, attended_all = lax.map(one_band, (windows, window_codes, keep_rows, band_counts))
    updated = results.reshape(N_BAND, win_rows, win_cols, WIN, WIN, CHAN).transpose(0, 1, 3, 2, 4, 5).reshape(height, WIDTH, CHAN)
    restored = jnp.roll(updated, (SHIFT, SHIFT), axis=(0, 1))
    tile_ids = jnp.arange(TILES_DEV, dtype=jnp.int32)
    tile_live = (tile_ids[None, :] * TILE < band_counts[:, None]) & (plan_slot < CAP)
    target = jnp.where(tile_live, plan_dest * CAP + plan_slot, N_BAND * CAP).astype(jnp.int32).reshape(-1)
    work_tiles = jnp.zeros((N_BAND * CAP + 1, TILE * WIN * WIN, CHAN), jnp.bfloat16)
    work_tiles = work_tiles.at[target].set(attended_all.reshape(-1, TILE * WIN * WIN, CHAN))[:N_BAND * CAP]
    return (restored, work_tiles)
```

```python
import functools

import jax
import jax.numpy as jnp
from jax import lax
from jax.experimental import pallas as pl
from jax.experimental.pallas import tpu as pltpu
from jax.sharding import PartitionSpec as P

CHAN = 180
HEADS = 6
HEAD_DIM = CHAN // HEADS
HEAD_PAD = 32
WIN = 8
TOKENS = WIN * WIN
TILE = 2
PAIR = TILE * TOKENS
SHIFT = 4
CAP = 8
TAIL = CHAN - 128
EPSILON = 1e-05

F32 = jnp.float32
BF16 = jnp.bfloat16


def dot(left, right, left_dim=1, right_dim=0):
    return lax.dot_general(
        left,
        right,
        (((left_dim,), (right_dim,)), ((), ())),
        preferred_element_type=F32,
    )


def layer_norm(values, gain):
    center = values - jnp.sum(values, axis=-1, keepdims=True) * (1.0 / CHAN)
    spread = jnp.sum(center * center, axis=-1, keepdims=True) * (1.0 / CHAN)
    return center * lax.rsqrt(spread + EPSILON) * gain


def region_mask(row_flag, col_flags):
    shape = (TOKENS, PAIR)
    key = lax.broadcasted_iota(jnp.int32, shape, 0)
    lane = lax.broadcasted_iota(jnp.int32, shape, 1)
    first = lane < TOKENS
    row_differs = ((key >> 5) & 1) ^ ((lane >> 5) & 1)
    col_differs = ((key >> 2) & 1) ^ ((lane >> 2) & 1)
    row_on = jnp.where(first, row_flag[0], row_flag[1])
    col_on = jnp.where(first, col_flags[0], col_flags[1])
    differs = (row_differs & row_on) | (col_differs & col_on)
    return jnp.where(differs == 1, -100.0, 0.0).astype(F32)


def attend(x, mask, bias_ref, gain, wqv_ref, wk_ref, proj_ref):
    normed = layer_norm(x, gain).astype(BF16)
    qv = dot(wqv_ref[...], normed, 1, 1)
    keys = dot(normed, wk_ref[...])
    lane = lax.broadcasted_iota(jnp.int32, (PAIR, PAIR), 1)
    key_low = (lane & 64) != 0
    first_lane = lax.broadcasted_iota(jnp.int32, (TOKENS, PAIR), 1) < TOKENS
    half = HEADS * HEAD_PAD
    mixed = []
    for head in range(HEADS):
        q = qv[head * HEAD_PAD : (head + 1) * HEAD_PAD] * (HEAD_DIM ** (-0.5))
        q_high = q.astype(BF16)
        q_low = (q - q_high.astype(F32)).astype(BF16)
        q_four = jnp.concatenate([q_high, q_low, q_high, q_low], axis=0)
        k = keys[:, head * PAIR : (head + 1) * PAIR]
        k_four = (k - jnp.where(key_low, k.astype(BF16).astype(F32), 0.0)).astype(BF16)
        scores = dot(k_four, q_four)
        scores = jnp.where(first_lane, scores[:TOKENS], scores[TOKENS:])
        scores = scores + bias_ref[head] + mask
        peak = jnp.max(scores, axis=0, keepdims=True)
        weights = jnp.exp(scores - peak)
        weights = weights * (1.0 / jnp.sum(weights, axis=0, keepdims=True))
        split = jnp.concatenate(
            [jnp.where(first_lane, weights, 0.0), jnp.where(first_lane, 0.0, weights)], axis=0
        ).astype(BF16)
        v = qv[half + head * HEAD_PAD : half + (head + 1) * HEAD_PAD].astype(BF16)
        mixed.append(dot(v, split))
    mixed = jnp.concatenate(mixed, axis=0).astype(BF16)
    return x + dot(mixed, proj_ref[...], 0, 0)


def feed(states, gain, hidden_ref, output_ref):
    normed = layer_norm(states, gain).astype(BF16)
    inner = jax.nn.gelu(dot(normed, hidden_ref[...]), approximate=True).astype(BF16)
    return states + dot(inner, output_ref[...])


def own_kernel(
    flags_ref,
    active_ref,
    x_ref,
    bias_ref,
    gain_attn_ref,
    wqv_ref,
    wk_ref,
    proj_ref,
    gain_mlp_ref,
    hidden_ref,
    output_ref,
    out_ref,
):
    step = pl.program_id(0)
    pairs = x_ref.shape[1] // (TILE * WIN)
    last = pl.num_programs(0) * pairs - 1
    for pair in range(pairs):
        columns = pl.ds(pair * TILE * WIN, TILE * WIN)
        block = x_ref[:, columns, :].astype(F32)
        x = jnp.concatenate(
            [
                block[:, w * WIN : (w + 1) * WIN].reshape(TOKENS, CHAN)
                for w in range(TILE)
            ],
            axis=0,
        )
        at_end = jnp.where(step * pairs + pair == last, 1, 0)
        row_flag = flags_ref[0]
        mask = region_mask((row_flag, row_flag), (0, at_end))
        attended = attend(x, mask, bias_ref, gain_attn_ref[...], wqv_ref, wk_ref, proj_ref)
        attended = attended.astype(BF16).astype(F32)
        done = feed(attended, gain_mlp_ref[...], hidden_ref, output_ref)
        parts = []
        for w in range(TILE):
            on = active_ref[(step * pairs + pair) * TILE + w]
            rows = slice(w * TOKENS, (w + 1) * TOKENS)
            parts.append(jnp.where(on == 1, done[rows], x[rows]).reshape(WIN, WIN, CHAN))
        out_ref[:, columns, :] = jnp.concatenate(parts, axis=1).astype(BF16)


def own_path(shifted, flags, active, bias, gain_attn, wqv, wk, proj, gain_mlp, hidden, output):
    rows, columns, _ = shifted.shape
    per_step = 2 * TILE * WIN
    whole = pl.BlockSpec(memory_space=pltpu.VMEM)
    scalars = pl.BlockSpec(memory_space=pltpu.SMEM)
    block = pl.BlockSpec((rows, per_step, CHAN), lambda i: (0, i, 0))
    return pl.pallas_call(
        own_kernel,
        grid=(columns // per_step,),
        in_specs=[scalars, scalars, block] + [whole] * 8,
        out_specs=block,
        out_shape=jax.ShapeDtypeStruct(shifted.shape, BF16),
        cost_estimate=pl.CostEstimate(
            flops=6_000_000_000, bytes_accessed=3_000_000, transcendentals=2_000_000
        ),
        name="own_path",
    )(flags, active, shifted, bias, gain_attn, wqv, wk, proj, gain_mlp, hidden, output)


def spread_kernel(pixels_ref, codes_ref, out_ref, heads, tails):
    rows, columns, _ = pixels_ref.shape
    tails[...] = jnp.zeros(tails.shape, F32)
    for row in range(rows):
        values = pixels_ref[row].astype(F32)
        heads[row, 0:columns, :] = values[:, 0:128]
        tails[row, 0:columns, 0:TAIL] = values[:, 128:CHAN]
        heads[row, columns : columns + WIN, :] = values[0:WIN, 0:128]
        tails[row, columns : columns + WIN, 0:TAIL] = values[0:WIN, 128:CHAN]
    codes = codes_ref[...]
    windows = columns // WIN
    half = windows // 2
    for token in range(TOKENS):
        row = (token // WIN + SHIFT) % rows
        picked = pl.ds(token % WIN + SHIFT, windows, stride=WIN)
        head = heads[row, picked, :]
        tail = tails[row, picked, :]
        packed = tail[:half] + pltpu.roll(tail[half:], TAIL, 1) + codes
        out_ref[token, :, 0:128] = head[:half].astype(BF16)
        out_ref[token, :, 128:256] = head[half:].astype(BF16)
        out_ref[token, :, 256:384] = packed.astype(BF16)


def spread(pixels, codes):
    rows, columns, _ = pixels.shape
    half = columns // WIN // 2
    return pl.pallas_call(
        spread_kernel,
        in_specs=[pl.BlockSpec(memory_space=pltpu.VMEM)] * 2,
        out_specs=pl.BlockSpec(memory_space=pltpu.VMEM),
        out_shape=jax.ShapeDtypeStruct((TOKENS, half, 384), BF16),
        scratch_shapes=[pltpu.VMEM((rows, columns + WIN, 128), F32)] * 2,
        cost_estimate=pl.CostEstimate(
            flops=100_000_000, bytes_accessed=2_000_000, transcendentals=0
        ),
        name="spread",
    )(pixels, codes)


def route_kernel(flags_ref, got_ref, out_ref):
    bands, half, _ = got_ref.shape
    slots = out_ref.shape[0] * out_ref.shape[1]
    sources = bands * half
    got = got_ref[...].reshape(sources, 384)
    tails = got[:, 256:384]
    row = lax.broadcasted_iota(jnp.int32, (8, 128), 0)
    lane = lax.broadcasted_iota(jnp.int32, (8, 128), 1) - 2 * TAIL - 2 * row
    pick = jnp.where(row < 2, jnp.where(lane == 0, 16.0, jnp.where(lane == 1, 1.0, 0.0)), 0.0)
    codes = dot(pick.astype(BF16), tails, 1, 1)
    codes = jnp.where(flags_ref[1] == 1, pltpu.roll(codes, half, 1), codes)
    low, high = codes[0:1].astype(jnp.int32), codes[1:2].astype(jnp.int32)
    chunk = 128
    lane_out = lax.broadcasted_iota(jnp.int32, (chunk, 128), 1)
    for start in range(0, slots, chunk):
        target = (lax.broadcasted_iota(jnp.int32, (chunk, sources), 0) + start) * TILE
        heads, tail_parts = [], []
        for place in range(TILE):
            pick_low = jnp.where(target + place == low, 1.0, 0.0).astype(BF16)
            pick_high = jnp.where(target + place == high, 1.0, 0.0).astype(BF16)
            first = jnp.concatenate([got[:, 0:128], tails], axis=1)
            second = jnp.concatenate([got[:, 128:256], tails], axis=1)
            from_low = dot(pick_low, first)
            from_high = dot(pick_high, second)
            heads.append(from_low[:, 0:128] + from_high[:, 0:128])
            low_tail, high_tail = from_low[:, 128:256], from_high[:, 128:256]
            high_moved = pltpu.roll(high_tail, 128 - TAIL, 1)
            tail = jnp.where(lane_out < TAIL, low_tail + high_moved, 0.0)
            kind_low = jnp.where(lane_out == 2 * TAIL + 4, low_tail, 0.0)
            kind_high = jnp.where(
                lane_out == 2 * TAIL + 4, pltpu.roll(high_tail, 127, 1), 0.0
            )
            kind = kind_low + kind_high
            if place:
                tail = pltpu.roll(tail, TAIL, 1)
                kind = pltpu.roll(kind, 1, 1)
            tail_parts.append(tail + kind)
        out = out_ref.at[start // CAP : (start + chunk) // CAP]
        blocks = chunk // CAP
        out[:, :, 0:128] = heads[0].reshape(blocks, CAP, 128).astype(BF16)
        out[:, :, 128:256] = heads[1].reshape(blocks, CAP, 128).astype(BF16)
        both = tail_parts[0] + tail_parts[1]
        out[:, :, 256:384] = both.reshape(blocks, CAP, 128).astype(BF16)


def route(got, flags):
    bands = got.shape[0]
    return pl.pallas_call(
        route_kernel,
        in_specs=[
            pl.BlockSpec(memory_space=pltpu.SMEM),
            pl.BlockSpec(memory_space=pltpu.VMEM),
        ],
        out_specs=pl.BlockSpec(memory_space=pltpu.VMEM),
        out_shape=jax.ShapeDtypeStruct((bands, CAP, 384), BF16),
        cost_estimate=pl.CostEstimate(
            flops=1_200_000_000, bytes_accessed=1_200_000, transcendentals=0
        ),
        name="route",
    )(flags, got)


def work_kernel(got_ref, kinds_ref, bias_ref, gain_ref, wqv_ref, wk_ref, proj_ref, out_ref, held):
    step = pl.program_id(0)

    @pl.when(step == 0)
    def _():
        for part in range(held.shape[0]):
            values = got_ref[:, :, part * 128 : (part + 1) * 128].astype(F32)
            held[part] = values.reshape(TOKENS * CAP, 128)

    slots = out_ref.shape[0]
    for index in range(slots):
        slot = step * slots + index
        rows = pl.ds(slot, TOKENS, stride=CAP)
        tail = held[TILE, rows, :]
        parts = []
        for place in range(TILE):
            head = held[place, rows, :]
            moved = pltpu.roll(tail, 128 - TAIL, 1) if place else tail
            parts.append(jnp.concatenate([head, moved], axis=1)[:, :CHAN])
        x = jnp.concatenate(parts, axis=0)
        kinds = [kinds_ref[slot * TILE + place] for place in range(TILE)]
        mask = region_mask([k & 1 for k in kinds], [k >> 1 for k in kinds])
        attended = attend(x, mask, bias_ref, gain_ref[...], wqv_ref, wk_ref, proj_ref)
        out_ref[index] = attended.astype(BF16)


def work_path(got, kinds, bias, gain, wqv, wk, proj):
    whole = pl.BlockSpec(memory_space=pltpu.VMEM)
    per_step = 2
    return pl.pallas_call(
        work_kernel,
        grid=(CAP // per_step,),
        in_specs=[whole, pl.BlockSpec(memory_space=pltpu.SMEM)] + [whole] * 5,
        out_specs=pl.BlockSpec((per_step, PAIR, CHAN), lambda i: (i, 0, 0)),
        out_shape=jax.ShapeDtypeStruct((CAP, PAIR, CHAN), BF16),
        scratch_shapes=[pltpu.VMEM((TILE + 1, TOKENS * CAP, 128), F32)],
        cost_estimate=pl.CostEstimate(
            flops=2_000_000_000, bytes_accessed=2_000_000, transcendentals=1_000_000
        ),
        name="work_path",
    )(got, kinds, bias, gain, wqv, wk, proj)


def from_behind(value, axis, steps):
    count = lax.axis_size(axis)
    pairs = [(source, (source + steps) % count) for source in range(count)]
    return lax.ppermute(value, axis, pairs)


def position_bias(bias_table):
    coords = jnp.arange(WIN, dtype=jnp.int32)
    offset = coords[None, :] - coords[:, None] + WIN - 1
    reach = 2 * WIN - 1
    onehot = (offset[:, :, None] == jnp.arange(reach)).astype(F32)
    table = bias_table.reshape(reach, reach, HEADS)
    looked = jnp.einsum(
        "kqa,abh->hkqb", onehot, table, precision=lax.Precision.HIGHEST
    )
    looked = jnp.einsum(
        "hkqb,cdb->hkcqd", looked, onehot, precision=lax.Precision.HIGHEST
    )
    looked = looked.reshape(HEADS, TOKENS, TOKENS)
    return jnp.concatenate([looked, looked], axis=2)


def pad_heads(weight):
    weight = weight.reshape(CHAN, HEADS, HEAD_DIM)
    return jnp.pad(weight, ((0, 0), (0, 0), (0, HEAD_PAD - HEAD_DIM)))


def shards(
    pixels,
    keep_mask,
    band_counts,
    plan_dest,
    plan_slot,
    bias_table,
    gain_attn,
    qkv_weight,
    proj_weight,
    gain_mlp,
    hidden_weight,
    output_weight,
):
    band_total = lax.axis_size("band")
    band_index = lax.axis_index("band")
    row_count, col_count, channels = pixels.shape
    window_total = (row_count // WIN) * (col_count // WIN)
    half = window_total // 2

    lower_rows = from_behind(pixels[:SHIFT], "band", -1)

    keep = keep_mask.reshape(window_total)
    position = jnp.cumsum(keep) - 1
    active = (keep == 1) & (position < band_counts[0])
    tile = position // TILE
    tile_onehot = tile[:, None] == jnp.arange(window_total // TILE)[None, :]
    dest = jnp.sum(jnp.where(tile_onehot, plan_dest, 0), axis=1)
    slot = jnp.sum(jnp.where(tile_onehot, plan_slot, 0), axis=1)
    placed = active & (slot < CAP)
    dest = jnp.where(placed, dest, band_total)
    place = jnp.where(placed, slot * TILE + position % TILE, 0)
    last_band = (band_index == band_total - 1).astype(jnp.int32)
    last_column = (jnp.arange(window_total) % (col_count // WIN) == col_count // WIN - 1)
    kind = last_band + 2 * last_column.astype(jnp.int32)
    codes = jnp.stack(
        [dest[:half], place[:half], dest[half:], place[half:], kind[:half], kind[half:]], axis=1
    )
    codes = jnp.pad(codes.astype(F32), ((0, 0), (2 * TAIL, 128 - 2 * TAIL - 6)))

    flags = jnp.stack([last_band, (band_index >= TOKENS // 2).astype(jnp.int32)])
    outgoing = spread(pixels, codes)
    gathered = lax.all_to_all(outgoing, "band", split_axis=0, concat_axis=0, tiled=True)

    bias = position_bias(bias_table)
    wq = pad_heads(qkv_weight[:, :CHAN]).reshape(CHAN, -1)
    wv = pad_heads(qkv_weight[:, 2 * CHAN :]).reshape(CHAN, -1)
    wqv = jnp.concatenate([wq, wv], axis=1).T
    wk = pad_heads(qkv_weight[:, CHAN : 2 * CHAN])
    wk = jnp.broadcast_to(wk[:, :, None, :], (CHAN, HEADS, 4, HEAD_PAD)).reshape(CHAN, -1)
    proj = jnp.pad(
        proj_weight.reshape(HEADS, HEAD_DIM, CHAN), ((0, 0), (0, HEAD_PAD - HEAD_DIM), (0, 0))
    ).reshape(HEADS * HEAD_PAD, CHAN)
    gain_one = gain_attn[None]

    shifted = jnp.roll(
        jnp.concatenate([pixels[SHIFT:], lower_rows], axis=0), -SHIFT, axis=1
    )
    band_shifted = own_path(
        shifted,
        flags,
        active.astype(jnp.int32),
        bias,
        gain_one,
        wqv,
        wk,
        proj,
        gain_mlp[None],
        hidden_weight,
        output_weight,
    )

    routed = route(gathered, flags)
    incoming = lax.all_to_all(routed, "band", split_axis=0, concat_axis=0, tiled=True)
    kinds = incoming[0, :, 256 + 2 * TAIL + 4 : 256 + 2 * TAIL + 6]
    kinds = kinds.astype(jnp.int32).reshape(CAP * TILE)
    work_tiles = work_path(incoming, kinds, bias, gain_one, wqv, wk, proj)

    band_shifted = jnp.roll(band_shifted, SHIFT, axis=1)
    upper_rows = from_behind(band_shifted[row_count - SHIFT :], "band", 1)
    restored = jnp.concatenate([upper_rows, band_shifted[: row_count - SHIFT]], axis=0)
    return (restored, work_tiles)


def solution(mesh):
    in_specs = (
        P(("img", "band"), None, None),
        P(("img", "band"), None),
        P(("img", "band")),
        P(("img", "band"), None),
        P(("img", "band"), None),
        P(),
        P(),
        P(),
        P(),
        P(),
        P(),
        P(),
    )
    out_specs = (P(("img", "band"), None, None), P(("img", "band"), None, None))
    return jax.shard_map(shards, mesh=mesh, in_specs=in_specs, out_specs=out_specs, check_vma=False)
```

```python
import jax
import jax.numpy as jnp
from jax import lax
from jax.experimental import pallas as pl
from jax.experimental.pallas import tpu as pltpu
from jax.sharding import PartitionSpec as P


CHAN = 180
HEADS = 6
HEAD_DIM = CHAN // HEADS
HEAD_PAD = 32
WIN = 8
TOKENS = WIN * WIN
TILE = 2
PAIR = TILE * TOKENS
SHIFT = 4
CAP = 8
TAIL = CHAN - 128
EPSILON = 1e-05

F32 = jnp.float32
BF16 = jnp.bfloat16


def dot(left, right, left_dim=1, right_dim=0):
    return lax.dot_general(
        left,
        right,
        (((left_dim,), (right_dim,)), ((), ())),
        preferred_element_type=F32,
    )


def layer_norm(values, gain):
    center = values - jnp.sum(values, axis=-1, keepdims=True) * (1.0 / CHAN)
    spread = jnp.sum(center * center, axis=-1, keepdims=True) * (1.0 / CHAN)
    return center * lax.rsqrt(spread + EPSILON) * gain


def iota(shape, dim):
    return lax.broadcasted_iota(jnp.int32, shape, dim)


def region_mask(row_flags, col_flags):
    shape = (TOKENS, PAIR)
    key, lane = iota(shape, 0), iota(shape, 1)
    first = lane < TOKENS
    row_differs = (((key >> 5) & 1) != ((lane >> 5) & 1)).astype(F32)
    col_differs = (((key >> 2) & 1) != ((lane >> 2) & 1)).astype(F32)
    row_on = jnp.where(first, row_flags[0], row_flags[1])
    col_on = jnp.where(first, col_flags[0], col_flags[1])
    return -100.0 * jnp.maximum(row_differs * row_on, col_differs * col_on)


def attend(x, masks, bias_ref, gain, wqv_ref, wk_ref):
    pairs = len(masks)
    normed = layer_norm(x, gain).astype(BF16)
    qv = dot(wqv_ref[...], normed, 1, 1)
    keys = dot(normed, wk_ref[...])
    key_low = (iota(keys.shape, 1) & 64) != 0
    keys = (keys - jnp.where(key_low, keys.astype(BF16).astype(F32), 0.0)).astype(BF16)
    half = HEADS * HEAD_PAD
    queries = qv[:half] * (HEAD_DIM ** (-0.5))
    high = queries.astype(BF16)
    low = (queries - high.astype(F32)).astype(BF16)
    values = qv[half:].astype(BF16)
    first_lane = iota((TOKENS, PAIR), 1) < TOKENS
    blank = jnp.zeros((PAIR, PAIR), BF16)
    scores = []
    for pair in range(pairs):
        lanes = slice(pair * PAIR, (pair + 1) * PAIR)
        for head in range(0, HEADS, 2):
            fours = []
            for one in (head, head + 1):
                rows = slice(one * HEAD_PAD, (one + 1) * HEAD_PAD)
                h, l = high[rows, lanes], low[rows, lanes]
                fours.append(jnp.concatenate([h, l, h, l], axis=0))
            both = jnp.concatenate(
                [
                    jnp.concatenate([fours[0], blank], axis=1),
                    jnp.concatenate([blank, fours[1]], axis=1),
                ],
                axis=0,
            )
            got = dot(keys[lanes, head * PAIR : (head + 2) * PAIR], both)
            for one in range(2):
                part = got[:, one * PAIR : (one + 1) * PAIR]
                scores.append(jnp.where(first_lane, part[:TOKENS], part[TOKENS:]))
    weights = []
    for pair in range(pairs):
        for head in range(HEADS):
            value = scores[pair * HEADS + head] + bias_ref[head] + masks[pair]
            value = jnp.exp(value - jnp.max(value, axis=0, keepdims=True))
            value = value * (1.0 / jnp.sum(value, axis=0, keepdims=True))
            weights.append(
                jnp.concatenate(
                    [jnp.where(first_lane, value, 0.0), jnp.where(first_lane, 0.0, value)], axis=0
                ).astype(BF16)
            )
    mixed = []
    for pair in range(pairs):
        lanes = slice(pair * PAIR, (pair + 1) * PAIR)
        parts = []
        for head in range(0, HEADS, 2):
            at = pair * HEADS + head
            both = jnp.concatenate([weights[at], weights[at + 1]], axis=1)
            rows = slice(head * HEAD_PAD, (head + 2) * HEAD_PAD)
            got = dot(values[rows, lanes], both)
            parts += [got[:HEAD_PAD, :PAIR], got[HEAD_PAD:, PAIR:]]
        mixed.append(jnp.concatenate(parts, axis=0).astype(BF16))
    return mixed


def feed(states, gain, hidden_ref, output_ref):
    normed = layer_norm(states, gain).astype(BF16)
    inner = jax.nn.gelu(dot(normed, hidden_ref[...]), approximate=True).astype(BF16)
    return states + dot(inner, output_ref[...])


VMEM = pl.BlockSpec(memory_space=pltpu.VMEM)
SMEM = pl.BlockSpec(memory_space=pltpu.SMEM)


def prep_kernel(
    qkv_ref, proj_ref, table_ref, wqv_ref, wk_ref, padded_ref, turned_ref, bias_ref, padded, looked
):
    half = HEADS * HEAD_PAD

    def source(column):
        inner = column & (HEAD_PAD - 1)
        return jnp.where(inner < HEAD_DIM, (column >> 5) * HEAD_DIM + inner, -1000)

    qkv = qkv_ref[...]
    column = iota((2 * half, 3 * CHAN), 0)
    wanted = jnp.where(column < half, source(column), 2 * CHAN + source(column - half))
    pick = (wanted == iota((2 * half, 3 * CHAN), 1)).astype(F32).astype(BF16)
    wqv_ref[...] = dot(pick, qkv, 1, 1).astype(BF16)
    shape = (3 * CHAN, HEADS * PAIR)
    column = iota(shape, 1)
    inner = column & (HEAD_PAD - 1)
    wanted = jnp.where(inner < HEAD_DIM, CHAN + (column >> 7) * HEAD_DIM + inner, -1)
    wk_ref[...] = dot(qkv, (wanted == iota(shape, 0)).astype(F32).astype(BF16)).astype(BF16)
    proj = proj_ref[...]
    pick = (source(iota((half, CHAN), 0)) == iota((half, CHAN), 1)).astype(F32).astype(BF16)
    padded_ref[...] = dot(pick, proj).astype(BF16)
    pick = (source(iota((CHAN, half), 1)) == iota((CHAN, half), 0)).astype(F32).astype(BF16)
    turned_ref[...] = dot(proj, pick, 0, 0).astype(BF16)

    reach = 2 * WIN - 1
    padded[...] = jnp.zeros(padded.shape, F32)
    padded[0:HEADS, 0 : reach * reach] = table_ref[...]
    table = padded[...]
    for key in range(TOKENS):
        shift = 112 - (key // WIN) * reach - key % WIN
        moved = pltpu.roll(table, (256 - shift) % 256, 1)[:, :PAIR]
        looked[key * 8 : (key + 1) * 8, :] = moved
    rest = looked[...]
    query = iota((PAIR, PAIR), 1) & (TOKENS - 1)
    pick = (iota((PAIR, PAIR), 0) == (query >> 3) * reach + (query & 7)).astype(F32).astype(BF16)
    total = None
    for _ in range(3):
        part = rest.astype(BF16)
        rest = rest - part.astype(F32)
        got = dot(part, pick)
        total = got if total is None else total + got
    looked[...] = total
    for head in range(HEADS):
        bias_ref[head] = looked[pl.ds(head, TOKENS, stride=8), :]


def prep(qkv_weight, proj_weight, table):
    half = HEADS * HEAD_PAD
    return pl.pallas_call(
        prep_kernel,
        in_specs=[VMEM] * 3,
        out_specs=[VMEM] * 5,
        out_shape=[
            jax.ShapeDtypeStruct((2 * half, CHAN), BF16),
            jax.ShapeDtypeStruct((CHAN, HEADS * PAIR), BF16),
            jax.ShapeDtypeStruct((half, CHAN), BF16),
            jax.ShapeDtypeStruct((CHAN, half), BF16),
            jax.ShapeDtypeStruct((HEADS, TOKENS, PAIR), F32),
        ],
        scratch_shapes=[pltpu.VMEM((8, 256), F32), pltpu.VMEM((8 * TOKENS, PAIR), F32)],
        cost_estimate=pl.CostEstimate(
            flops=600_000_000, bytes_accessed=1_500_000, transcendentals=0
        ),
        name="prep",
    )(qkv_weight, proj_weight, table)


def own_kernel(
    keep_ref,
    count_ref,
    rest_ref,
    halo_ref,
    bias_ref,
    gain_attn_ref,
    wqv_ref,
    wk_ref,
    proj_ref,
    gain_mlp_ref,
    hidden_ref,
    output_ref,
    out_ref,
    send_ref,
    active,
):
    step = pl.program_id(0)
    steps = pl.num_programs(0)
    pairs = rest_ref.shape[1] // (TILE * WIN)
    row_flag = jnp.where(lax.axis_index("band") == lax.axis_size("band") - 1, 1.0, 0.0)

    @pl.when(step == 0)
    def _():
        position = jnp.int32(-1)
        for w in range(keep_ref.shape[1]):
            keep = keep_ref[0, w]
            position = position + keep
            active[w] = jnp.where((keep == 1) & (position < count_ref[0]), 1, 0)

    tokens, masks = [], []
    for pair in range(pairs):
        columns = pl.ds(pair * TILE * WIN, TILE * WIN)
        upper = rest_ref[:, columns, :].astype(F32)
        lower = halo_ref[:, columns, :].astype(F32)
        for w in range(TILE):
            for part in (upper, lower):
                tokens.append(
                    part[:, w * WIN : (w + 1) * WIN].reshape(SHIFT * WIN, CHAN)
                )
        at_end = jnp.where((step == steps - 1) & (pair == pairs - 1), 1.0, 0.0)
        masks.append(region_mask((row_flag, row_flag), (0.0, at_end)))
    x = jnp.concatenate(tokens, axis=0)
    mixed = attend(x, masks, bias_ref, gain_attn_ref[...], wqv_ref, wk_ref)
    projected = [dot(part, proj_ref[...], 0, 0) for part in mixed]
    attended = x + jnp.concatenate(projected, axis=0)
    attended = attended.astype(BF16).astype(F32)
    done = feed(attended, gain_mlp_ref[...], hidden_ref, output_ref)
    for pair in range(pairs):
        columns = pl.ds(pair * TILE * WIN, TILE * WIN)
        uppers, lowers = [], []
        for w in range(TILE):
            at = pair * TILE + w
            on = active[step * pairs * TILE + at]
            rows = slice(at * TOKENS, (at + 1) * TOKENS)
            kept = jnp.where(on == 1, done[rows], x[rows]).reshape(WIN, WIN, CHAN)
            uppers.append(kept[:SHIFT])
            lowers.append(kept[SHIFT:])
        out_ref[:, columns, :] = jnp.concatenate(uppers, axis=1).astype(BF16)
        send_ref[:, columns, :] = jnp.concatenate(lowers, axis=1).astype(BF16)


def own_path(keep, count, rest, halo, bias, gain_attn, wqv, wk, proj, gain_mlp, hidden, output):
    rows, columns, _ = rest.shape
    per_step = 2 * TILE * WIN
    block = pl.BlockSpec((rows, per_step, CHAN), lambda i: (0, i, 0))
    return pl.pallas_call(
        own_kernel,
        grid=(columns // per_step,),
        in_specs=[SMEM, SMEM, block, block] + [VMEM] * 8,
        out_specs=[block, block],
        out_shape=[jax.ShapeDtypeStruct(rest.shape, BF16)] * 2,
        scratch_shapes=[pltpu.SMEM((columns // WIN,), jnp.int32)],
        cost_estimate=pl.CostEstimate(
            flops=20_000_000_000, bytes_accessed=3_000_000, transcendentals=2_000_000
        ),
        name="own_path",
    )(keep, count, rest, halo, bias, gain_attn, wqv, wk, proj, gain_mlp, hidden, output)


def spread_kernel(
    keep_ref, count_ref, dest_ref, slot_ref, pixels_ref, out_ref, top_ref, rest_ref, heads, tails
):
    rows, columns, _ = pixels_ref.shape
    windows = columns // WIN
    half = windows // 2
    bands = lax.axis_size("band")
    last_band = jnp.where(lax.axis_index("band") == bands - 1, 1.0, 0.0)
    row, lane = iota((half, 128), 0), iota((half, 128), 1) - 2 * TAIL
    codes = jnp.where((lane == 4) | (lane == 6), last_band, 0.0)
    codes = jnp.where((lane == 7) & (row == half - 1), 1.0, codes)
    position = jnp.int32(-1)
    for w in range(windows):
        keep = keep_ref[0, w]
        position = position + keep
        tile = jnp.maximum(position, 0) >> 1
        slot = slot_ref[0, tile]
        placed = (keep == 1) & (position < count_ref[0]) & (slot < CAP)
        dest = jnp.where(placed, dest_ref[0, tile], bands).astype(F32)
        place = jnp.where(placed, slot * TILE + (position & 1), 0).astype(F32)
        first = 2 * (w // half)
        here = row == w % half
        codes = jnp.where(here & (lane == first), dest, codes)
        codes = jnp.where(here & (lane == first + 1), place, codes)

    tails[...] = jnp.zeros(tails.shape, F32)
    for r in range(rows):
        values = pixels_ref[r].astype(F32)
        heads[r, 0:columns, :] = values[:, 0:128]
        tails[r, 0:columns, 0:TAIL] = values[:, 128:CHAN]
        heads[r, columns : columns + WIN, :] = values[0:WIN, 0:128]
        tails[r, columns : columns + WIN, 0:TAIL] = values[0:WIN, 128:CHAN]
    for r in range(rows):
        target = top_ref.at[r] if r < SHIFT else rest_ref.at[r - SHIFT]
        target[:, 0:128] = heads[r, SHIFT : SHIFT + columns, :].astype(BF16)
        target[:, 128:CHAN] = tails[r, SHIFT : SHIFT + columns, 0:TAIL].astype(BF16)
    for token in range(TOKENS):
        r = (token // WIN + SHIFT) % rows
        picked = pl.ds(token % WIN + SHIFT, windows, stride=WIN)
        head = heads[r, picked, :]
        tail = tails[r, picked, :]
        packed = tail[:half] + pltpu.roll(tail[half:], TAIL, 1) + codes
        out_ref[token, :, 0:128] = head[:half].astype(BF16)
        out_ref[token, :, 128:256] = head[half:].astype(BF16)
        out_ref[token, :, 256:384] = packed.astype(BF16)


def spread(keep, count, dest, slot, pixels):
    rows, columns, _ = pixels.shape
    half = columns // WIN // 2
    part = jax.ShapeDtypeStruct((SHIFT, columns, CHAN), BF16)
    return pl.pallas_call(
        spread_kernel,
        in_specs=[SMEM] * 4 + [VMEM],
        out_specs=[VMEM] * 3,
        out_shape=[jax.ShapeDtypeStruct((TOKENS, half, 384), BF16), part, part],
        scratch_shapes=[pltpu.VMEM((rows, columns + WIN, 128), F32)] * 2,
        cost_estimate=pl.CostEstimate(
            flops=100_000_000, bytes_accessed=2_000_000, transcendentals=0
        ),
        name="spread",
    )(keep, count, dest, slot, pixels)


def route_kernel(got_ref, out_ref):
    bands, half, _ = got_ref.shape
    slots = out_ref.shape[0] * out_ref.shape[1]
    sources = bands * half
    got = got_ref[...].reshape(sources, 384)
    tails = got[:, 256:384]
    row = iota((8, 128), 0)
    lane = iota((8, 128), 1) - 2 * TAIL - 2 * row
    pick = jnp.where(row < 2, jnp.where(lane == 0, 16.0, jnp.where(lane == 1, 1.0, 0.0)), 0.0)
    codes = dot(pick.astype(BF16), tails, 1, 1)
    behind = lax.axis_index("band") >= TOKENS // 2
    codes = jnp.where(behind, pltpu.roll(codes, half, 1), codes)
    low, high = codes[0:1].astype(jnp.int32), codes[1:2].astype(jnp.int32)
    chunk = 128
    lane_out = iota((chunk, 128), 1)
    is_kind = (lane_out == 2 * TAIL + 4) | (lane_out == 2 * TAIL + 5)
    first = jnp.concatenate([got[:, 0:128], tails], axis=1)
    second = jnp.concatenate([got[:, 128:256], tails], axis=1)
    for start in range(0, slots, chunk):
        target = (iota((chunk, sources), 0) + start) * TILE
        heads, total = [], None
        for place in range(TILE):
            pick_low = jnp.where(target + place == low, 1.0, 0.0).astype(BF16)
            pick_high = jnp.where(target + place == high, 1.0, 0.0).astype(BF16)
            from_low = dot(pick_low, first)
            from_high = dot(pick_high, second)
            heads.append(from_low[:, 0:128] + from_high[:, 0:128])
            low_tail, high_tail = from_low[:, 128:256], from_high[:, 128:256]
            tail = low_tail + pltpu.roll(high_tail, 128 - TAIL, 1)
            kind = low_tail + pltpu.roll(high_tail, 126, 1)
            tail = jnp.where(lane_out < TAIL, tail, 0.0)
            kind = jnp.where(is_kind, kind, 0.0)
            if place:
                tail = pltpu.roll(tail, TAIL, 1)
                kind = pltpu.roll(kind, 2, 1)
            total = tail + kind if total is None else total + tail + kind
        out = out_ref.at[start // CAP : (start + chunk) // CAP]
        blocks = chunk // CAP
        out[:, :, 0:128] = heads[0].reshape(blocks, CAP, 128).astype(BF16)
        out[:, :, 128:256] = heads[1].reshape(blocks, CAP, 128).astype(BF16)
        out[:, :, 256:384] = total.reshape(blocks, CAP, 128).astype(BF16)


def route(got):
    bands = got.shape[0]
    return pl.pallas_call(
        route_kernel,
        in_specs=[VMEM],
        out_specs=VMEM,
        out_shape=jax.ShapeDtypeStruct((bands, CAP, 384), BF16),
        cost_estimate=pl.CostEstimate(
            flops=1_200_000_000, bytes_accessed=1_200_000, transcendentals=0
        ),
        name="route",
    )(got)


def work_kernel(got_ref, bias_ref, gain_ref, wqv_ref, wk_ref, proj_ref, out_ref, held, done):
    for part in range(held.shape[0]):
        values = got_ref[:, :, part * 128 : (part + 1) * 128].astype(F32)
        held[part] = values.reshape(TOKENS * CAP, 128)
    pairs = 2

    def two_slots(step, carry):
        tokens, masks = [], []
        for index in range(pairs):
            slot = step * pairs + index
            rows = pl.ds(slot, TOKENS, stride=CAP)
            tail = held[TILE, rows, :]
            for place in range(TILE):
                head = held[place, rows, :]
                moved = pltpu.roll(tail, 128 - TAIL, 1) if place else tail
                tokens.append(jnp.concatenate([head, moved], axis=1)[:, :CHAN])
            lane = iota((1, 128), 1) - 2 * TAIL - 4
            flags = [
                jnp.sum(jnp.where(lane == i, tail[0:1], 0.0), axis=1, keepdims=True)
                for i in range(4)
            ]
            masks.append(region_mask(flags[0::2], flags[1::2]))
        x = jnp.concatenate(tokens, axis=0)
        mixed = attend(x, masks, bias_ref, gain_ref[...], wqv_ref, wk_ref)
        for index in range(pairs):
            rows = pl.ds(step * pairs + index, CHAN, stride=CAP)
            own = x[index * PAIR : (index + 1) * PAIR]
            done[rows, :] = own.T + dot(proj_ref[...], mixed[index])
        return carry

    lax.fori_loop(0, CAP // pairs, two_slots, 0)
    out_ref[...] = done[...].reshape(CHAN, CAP, PAIR).astype(BF16)


def work_path(got, bias, gain, wqv, wk, proj):
    return pl.pallas_call(
        work_kernel,
        in_specs=[VMEM] * 6,
        out_specs=VMEM,
        out_shape=jax.ShapeDtypeStruct((CHAN, CAP, PAIR), BF16),
        scratch_shapes=[
            pltpu.VMEM((TILE + 1, TOKENS * CAP, 128), F32),
            pltpu.VMEM((CHAN * CAP, PAIR), F32),
        ],
        cost_estimate=pl.CostEstimate(
            flops=8_000_000_000, bytes_accessed=2_000_000, transcendentals=1_000_000
        ),
        name="work_path",
    )(got, bias, gain, wqv, wk, proj)


def from_behind(value, axis, steps):
    count = lax.axis_size(axis)
    pairs = [(source, (source + steps) % count) for source in range(count)]
    return lax.ppermute(value, axis, pairs)


def shards(
    pixels,
    keep_mask,
    band_counts,
    plan_dest,
    plan_slot,
    bias_table,
    gain_attn,
    qkv_weight,
    proj_weight,
    gain_mlp,
    hidden_weight,
    output_weight,
):
    gain_attn, gain_mlp = gain_attn[None], gain_mlp[None]
    outgoing, top, rest = spread(keep_mask, band_counts, plan_dest, plan_slot, pixels)
    halo = from_behind(top, "band", -1)
    gathered = lax.all_to_all(outgoing, "band", split_axis=0, concat_axis=0, tiled=True)
    wqv, wk, proj, proj_turned, bias = prep(qkv_weight, proj_weight, bias_table.T)
    kept, sent = own_path(
        keep_mask,
        band_counts,
        rest,
        halo,
        bias,
        gain_attn,
        wqv,
        wk,
        proj,
        gain_mlp,
        hidden_weight,
        output_weight,
    )
    upper = from_behind(sent, "band", 1)
    routed = route(gathered)
    incoming = lax.all_to_all(routed, "band", split_axis=0, concat_axis=0, tiled=True)
    restored = jnp.roll(jnp.concatenate([upper, kept], axis=0), SHIFT, axis=1)
    work_tiles = work_path(incoming, bias, gain_attn, wqv, wk, proj_turned)
    work_tiles = jnp.transpose(work_tiles, (1, 2, 0))
    return (restored, work_tiles)


def solution(mesh):
    in_specs = (
        P(("img", "band"), None, None),
        P(("img", "band"), None),
        P(("img", "band")),
        P(("img", "band"), None),
        P(("img", "band"), None),
        P(),
        P(),
        P(),
        P(),
        P(),
        P(),
        P(),
    )
    out_specs = (P(("img", "band"), None, None), P(("img", "band"), None, None))
    return jax.shard_map(shards, mesh=mesh, in_specs=in_specs, out_specs=out_specs, check_vma=False)
```

```python
import jax
import jax.numpy as jnp
from jax import lax
from jax.experimental import pallas as pl
from jax.experimental.pallas import tpu as pltpu
from jax.sharding import PartitionSpec as P


CHAN = 180
HEADS = 6
HEAD_DIM = CHAN // HEADS
HEAD_PAD = 32
WIN = 8
TOKENS = WIN * WIN
TILE = 2
PAIR = TILE * TOKENS
SHIFT = 4
CAP = 8
TAIL = CHAN - 128
EPSILON = 1e-05

F32 = jnp.float32
BF16 = jnp.bfloat16


def dot(left, right, left_dim=1, right_dim=0):
    return lax.dot_general(
        left,
        right,
        (((left_dim,), (right_dim,)), ((), ())),
        preferred_element_type=F32,
    )


def layer_norm(values, gain):
    center = values - jnp.sum(values, axis=-1, keepdims=True) * (1.0 / CHAN)
    spread = jnp.sum(center * center, axis=-1, keepdims=True) * (1.0 / CHAN)
    return center * lax.rsqrt(spread + EPSILON) * gain


def iota(shape, dim):
    return lax.broadcasted_iota(jnp.int32, shape, dim)


def region_mask(row_flags, col_flags):
    shape = (TOKENS, PAIR)
    key, lane = iota(shape, 0), iota(shape, 1)
    first = lane < TOKENS
    row_differs = (((key >> 5) & 1) != ((lane >> 5) & 1)).astype(F32)
    col_differs = (((key >> 2) & 1) != ((lane >> 2) & 1)).astype(F32)
    row_on = jnp.where(first, row_flags[0], row_flags[1])
    col_on = jnp.where(first, col_flags[0], col_flags[1])
    return -100.0 * jnp.maximum(row_differs * row_on, col_differs * col_on)


def attend(x, masks, bias_ref, gain, wqv_ref, wk_ref):
    pairs = len(masks)
    normed = layer_norm(x, gain).astype(BF16)
    qv = dot(wqv_ref[...], normed, 1, 1)
    keys = dot(normed, wk_ref[...])
    key_low = (iota(keys.shape, 1) & 64) != 0
    keys = (keys - jnp.where(key_low, keys.astype(BF16).astype(F32), 0.0)).astype(BF16)
    half = HEADS * HEAD_PAD
    queries = qv[:half] * (HEAD_DIM ** (-0.5))
    high = queries.astype(BF16)
    low = (queries - high.astype(F32)).astype(BF16)
    values = qv[half:].astype(BF16)
    first_lane = iota((TOKENS, PAIR), 1) < TOKENS
    blank = jnp.zeros((PAIR, PAIR), BF16)
    scores = []
    for pair in range(pairs):
        lanes = slice(pair * PAIR, (pair + 1) * PAIR)
        for head in range(0, HEADS, 2):
            fours = []
            for one in (head, head + 1):
                rows = slice(one * HEAD_PAD, (one + 1) * HEAD_PAD)
                h, l = high[rows, lanes], low[rows, lanes]
                fours.append(jnp.concatenate([h, l, h, l], axis=0))
            both = jnp.concatenate(
                [
                    jnp.concatenate([fours[0], blank], axis=1),
                    jnp.concatenate([blank, fours[1]], axis=1),
                ],
                axis=0,
            )
            got = dot(keys[lanes, head * PAIR : (head + 2) * PAIR], both)
            for one in range(2):
                part = got[:, one * PAIR : (one + 1) * PAIR]
                scores.append(jnp.where(first_lane, part[:TOKENS], part[TOKENS:]))
    weights = []
    for pair in range(pairs):
        for head in range(HEADS):
            value = scores[pair * HEADS + head] + bias_ref[head] + masks[pair]
            value = jnp.exp(value - jnp.max(value, axis=0, keepdims=True))
            value = value * (1.0 / jnp.sum(value, axis=0, keepdims=True))
            weights.append(
                jnp.concatenate(
                    [jnp.where(first_lane, value, 0.0), jnp.where(first_lane, 0.0, value)], axis=0
                ).astype(BF16)
            )
    mixed = []
    for pair in range(pairs):
        lanes = slice(pair * PAIR, (pair + 1) * PAIR)
        parts = []
        for head in range(0, HEADS, 2):
            at = pair * HEADS + head
            both = jnp.concatenate([weights[at], weights[at + 1]], axis=1)
            rows = slice(head * HEAD_PAD, (head + 2) * HEAD_PAD)
            got = dot(values[rows, lanes], both)
            parts += [got[:HEAD_PAD, :PAIR], got[HEAD_PAD:, PAIR:]]
        mixed.append(jnp.concatenate(parts, axis=0).astype(BF16))
    return mixed


def feed(states, gain, hidden_ref, output_ref):
    normed = layer_norm(states, gain).astype(BF16)
    inner = jax.nn.gelu(dot(normed, hidden_ref[...]), approximate=True).astype(BF16)
    return states + dot(inner, output_ref[...], 1, 1)


VMEM = pl.BlockSpec(memory_space=pltpu.VMEM)
SMEM = pl.BlockSpec(memory_space=pltpu.SMEM)


def prep_kernel(
    qkv_ref, proj_ref, table_ref, wqv_ref, wk_ref, padded_ref, turned_ref, bias_ref, padded, looked
):
    half = HEADS * HEAD_PAD

    def source(column):
        inner = column & (HEAD_PAD - 1)
        return jnp.where(inner < HEAD_DIM, (column >> 5) * HEAD_DIM + inner, -1000)

    qkv = qkv_ref[...]
    column = iota((2 * half, 3 * CHAN), 0)
    wanted = jnp.where(column < half, source(column), 2 * CHAN + source(column - half))
    pick = (wanted == iota((2 * half, 3 * CHAN), 1)).astype(F32).astype(BF16)
    wqv_ref[...] = dot(pick, qkv, 1, 1).astype(BF16)
    shape = (3 * CHAN, HEADS * PAIR)
    column = iota(shape, 1)
    inner = column & (HEAD_PAD - 1)
    wanted = jnp.where(inner < HEAD_DIM, CHAN + (column >> 7) * HEAD_DIM + inner, -1)
    wk_ref[...] = dot(qkv, (wanted == iota(shape, 0)).astype(F32).astype(BF16)).astype(BF16)
    proj = proj_ref[...]
    pick = (source(iota((half, CHAN), 0)) == iota((half, CHAN), 1)).astype(F32).astype(BF16)
    padded_ref[...] = dot(pick, proj).astype(BF16)
    pick = (source(iota((CHAN, half), 1)) == iota((CHAN, half), 0)).astype(F32).astype(BF16)
    turned_ref[...] = dot(proj, pick, 0, 0).astype(BF16)

    reach = 2 * WIN - 1
    padded[...] = jnp.zeros(padded.shape, F32)
    padded[0:HEADS, 0 : reach * reach] = table_ref[...]
    table = padded[...]
    for key in range(TOKENS):
        shift = 112 - (key // WIN) * reach - key % WIN
        moved = pltpu.roll(table, (256 - shift) % 256, 1)[:, :PAIR]
        looked[key * 8 : (key + 1) * 8, :] = moved
    rest = looked[...]
    query = iota((PAIR, PAIR), 1) & (TOKENS - 1)
    pick = (iota((PAIR, PAIR), 0) == (query >> 3) * reach + (query & 7)).astype(F32).astype(BF16)
    total = None
    for _ in range(3):
        part = rest.astype(BF16)
        rest = rest - part.astype(F32)
        got = dot(part, pick)
        total = got if total is None else total + got
    looked[...] = total
    for head in range(HEADS):
        bias_ref[head] = looked[pl.ds(head, TOKENS, stride=8), :]


def prep(qkv_weight, proj_weight, table):
    half = HEADS * HEAD_PAD
    return pl.pallas_call(
        prep_kernel,
        in_specs=[VMEM] * 3,
        out_specs=[VMEM] * 5,
        out_shape=[
            jax.ShapeDtypeStruct((2 * half, CHAN), BF16),
            jax.ShapeDtypeStruct((CHAN, HEADS * PAIR), BF16),
            jax.ShapeDtypeStruct((half, CHAN), BF16),
            jax.ShapeDtypeStruct((CHAN, half), BF16),
            jax.ShapeDtypeStruct((HEADS, TOKENS, PAIR), F32),
        ],
        scratch_shapes=[pltpu.VMEM((8, 256), F32), pltpu.VMEM((8 * TOKENS, PAIR), F32)],
        cost_estimate=pl.CostEstimate(
            flops=600_000_000, bytes_accessed=1_500_000, transcendentals=0
        ),
        name="prep",
    )(qkv_weight, proj_weight, table)


def turned_rows(flat, row, stride):
    rows = pl.ds(row, 256, stride=stride)
    return jnp.concatenate([half[rows, :] for half in flat], axis=1).astype(BF16)


def hold_channels(block_ref, flat):
    channels, rows, _ = block_ref.shape
    for index, half in enumerate(flat):
        values = block_ref[:, :, index * 128 : (index + 1) * 128].astype(F32)
        half[0 : channels * rows, :] = values.reshape(channels * rows, 128)
        half[channels * rows :, :] = jnp.zeros((half.shape[0] - channels * rows, 128), F32)


def roll_pick(columns):
    wanted = (iota((columns, columns), 0) + SHIFT) & (columns - 1)
    return (wanted == iota((columns, columns), 1)).astype(F32).astype(BF16)


def own_kernel(
    keep_ref,
    count_ref,
    rest_ref,
    halo_ref,
    bias_ref,
    gain_attn_ref,
    wqv_ref,
    wk_ref,
    proj_ref,
    gain_mlp_ref,
    hidden_ref,
    output_ref,
    out_ref,
    active,
    flat0,
    flat1,
    lower_rows,
    finished,
    turned0,
    turned1,
):
    step = pl.program_id(0)
    steps = pl.num_programs(0)
    columns_all = out_ref.shape[2]
    pairs = rest_ref.shape[1] // (TILE * WIN)
    row_flag = jnp.where(lax.axis_index("band") == lax.axis_size("band") - 1, 1.0, 0.0)

    @pl.when(step == 0)
    def _():
        position = jnp.int32(-1)
        for w in range(keep_ref.shape[1]):
            keep = keep_ref[0, w]
            position = position + keep
            active[w] = jnp.where((keep == 1) & (position < count_ref[0]), 1, 0)
        hold_channels(halo_ref, (flat0, flat1))
        pick = roll_pick(columns_all)
        for row in range(SHIFT):
            got = dot(pick, turned_rows((flat0, flat1), row, SHIFT), 1, 1)
            lower_rows[row] = got[:, :CHAN]

    tokens, masks = [], []
    for pair in range(pairs):
        columns = pl.ds(pair * TILE * WIN, TILE * WIN)
        start = pl.multiple_of((step * pairs + pair) * TILE * WIN, TILE * WIN)
        upper = rest_ref[:, columns, :].astype(F32)
        lower = lower_rows[:, pl.ds(start, TILE * WIN), :]
        for w in range(TILE):
            for part in (upper, lower):
                tokens.append(
                    part[:, w * WIN : (w + 1) * WIN].reshape(SHIFT * WIN, CHAN)
                )
        at_end = jnp.where((step == steps - 1) & (pair == pairs - 1), 1.0, 0.0)
        masks.append(region_mask((row_flag, row_flag), (0.0, at_end)))
    x = jnp.concatenate(tokens, axis=0)
    mixed = attend(x, masks, bias_ref, gain_attn_ref[...], wqv_ref, wk_ref)
    projected = [dot(part, proj_ref[...], 0, 0) for part in mixed]
    attended = x + jnp.concatenate(projected, axis=0)
    attended = attended.astype(BF16).astype(F32)
    done = feed(attended, gain_mlp_ref[...], hidden_ref, output_ref)
    for pair in range(pairs):
        start = pl.multiple_of((step * pairs + pair) * TILE * WIN, TILE * WIN)
        kept = []
        for w in range(TILE):
            at = pair * TILE + w
            on = active[step * pairs * TILE + at]
            rows = slice(at * TOKENS, (at + 1) * TOKENS)
            kept.append(jnp.where(on == 1, done[rows], x[rows]).reshape(WIN, WIN, CHAN))
        kept = jnp.concatenate(kept, axis=1).astype(BF16)
        finished[:, pl.ds(start, TILE * WIN), :] = kept

    @pl.when(step == steps - 1)
    def _():
        same = (iota((CHAN, CHAN), 0) == iota((CHAN, CHAN), 1)).astype(F32).astype(BF16)
        for row in range(WIN):
            got = dot(same, finished[(row + SHIFT) % WIN], 1, 1)
            got = pltpu.roll(got, SHIFT, 1)
            rows = pl.ds(row, CHAN, stride=WIN)
            turned0[rows, :] = got[:, :128]
            turned1[rows, :] = got[:, 128:]
        out_ref[:, :, 0:128] = turned0[...].reshape(CHAN, WIN, 128).astype(BF16)
        out_ref[:, :, 128:256] = turned1[...].reshape(CHAN, WIN, 128).astype(BF16)


def own_path(keep, count, rest, halo, bias, gain_attn, wqv, wk, proj, gain_mlp, hidden, output):
    rows, columns, _ = rest.shape
    per_step = 2 * TILE * WIN
    block = pl.BlockSpec((rows, per_step, CHAN), lambda i: (0, i, 0))
    flat = pltpu.VMEM((256 * SHIFT, 128), F32)
    turned = pltpu.VMEM((CHAN * WIN, 128), F32)
    return pl.pallas_call(
        own_kernel,
        grid=(columns // per_step,),
        in_specs=[SMEM, SMEM, block] + [VMEM] * 9,
        out_specs=VMEM,
        out_shape=jax.ShapeDtypeStruct((CHAN, WIN, columns), BF16),
        scratch_shapes=[
            pltpu.SMEM((columns // WIN,), jnp.int32),
            flat,
            flat,
            pltpu.VMEM((SHIFT, columns, CHAN), F32),
            pltpu.VMEM((WIN, columns, CHAN), BF16),
            turned,
            turned,
        ],
        cost_estimate=pl.CostEstimate(
            flops=20_000_000_000, bytes_accessed=3_000_000, transcendentals=2_000_000
        ),
        name="own_path",
    )(keep, count, rest, halo, bias, gain_attn, wqv, wk, proj, gain_mlp, hidden, output)


def spread_kernel(
    keep_ref, count_ref, dest_ref, slot_ref, pixels_ref, out_ref, rest_ref, flat0, flat1
):
    _, rows, columns = pixels_ref.shape
    windows = columns // WIN
    half = windows // 2
    bands = lax.axis_size("band")
    last_band = jnp.where(lax.axis_index("band") == bands - 1, 1.0, 0.0)
    row, lane = iota((half, 128), 0), iota((half, 128), 1) - 2 * TAIL
    codes = jnp.where((lane == 4) | (lane == 6), last_band, 0.0)
    codes = jnp.where((lane == 7) & (row == half - 1), 1.0, codes)
    position = jnp.int32(-1)
    for w in range(windows):
        keep = keep_ref[0, w]
        position = position + keep
        tile = jnp.maximum(position, 0) >> 1
        slot = slot_ref[0, tile]
        placed = (keep == 1) & (position < count_ref[0]) & (slot < CAP)
        dest = jnp.where(placed, dest_ref[0, tile], bands).astype(F32)
        place = jnp.where(placed, slot * TILE + (position & 1), 0).astype(F32)
        first = 2 * (w // half)
        here = row == w % half
        codes = jnp.where(here & (lane == first), dest, codes)
        codes = jnp.where(here & (lane == first + 1), place, codes)

    hold_channels(pixels_ref, (flat0, flat1))
    out_row = iota((columns, columns), 0)
    wanted = ((out_row & (windows - 1)) * WIN + (out_row >> 5) + SHIFT) & (columns - 1)
    group = (wanted == iota((columns, columns), 1)).astype(F32).astype(BF16)
    pick = roll_pick(columns)
    for r in range(rows):
        line = turned_rows((flat0, flat1), r, rows)
        if r >= SHIFT:
            rest_ref[r - SHIFT] = dot(pick, line, 1, 1)[:, :CHAN].astype(BF16)
        got = dot(group, line, 1, 1)
        for cu in range(WIN):
            token = (r + SHIFT) % rows * WIN + cu
            low = got[cu * windows : cu * windows + half]
            high = got[cu * windows + half : (cu + 1) * windows]
            packed = low[:, 128:] + pltpu.roll(high[:, 128:], TAIL, 1) + codes
            out_ref[token, :, 0:128] = low[:, :128].astype(BF16)
            out_ref[token, :, 128:256] = high[:, :128].astype(BF16)
            out_ref[token, :, 256:384] = packed.astype(BF16)


def spread(keep, count, dest, slot, pixels):
    _, rows, columns = pixels.shape
    half = columns // WIN // 2
    flat = pltpu.VMEM((256 * rows, 128), F32)
    return pl.pallas_call(
        spread_kernel,
        in_specs=[SMEM] * 4 + [VMEM],
        out_specs=[VMEM] * 2,
        out_shape=[
            jax.ShapeDtypeStruct((TOKENS, half, 384), BF16),
            jax.ShapeDtypeStruct((SHIFT, columns, CHAN), BF16),
        ],
        scratch_shapes=[flat, flat],
        cost_estimate=pl.CostEstimate(
            flops=500_000_000, bytes_accessed=2_000_000, transcendentals=0
        ),
        name="spread",
    )(keep, count, dest, slot, pixels)


def route_kernel(got_ref, out_ref):
    bands, half, _ = got_ref.shape
    slots = out_ref.shape[0] * out_ref.shape[1]
    sources = bands * half
    got = got_ref[...].reshape(sources, 384)
    tails = got[:, 256:384]
    row = iota((8, 128), 0)
    lane = iota((8, 128), 1) - 2 * TAIL - 2 * row
    pick = jnp.where(row < 2, jnp.where(lane == 0, 16.0, jnp.where(lane == 1, 1.0, 0.0)), 0.0)
    codes = dot(pick.astype(BF16), tails, 1, 1)
    behind = lax.axis_index("band") >= TOKENS // 2
    codes = jnp.where(behind, pltpu.roll(codes, half, 1), codes)
    low, high = codes[0:1].astype(jnp.int32), codes[1:2].astype(jnp.int32)
    chunk = 128
    lane_out = iota((chunk, 128), 1)
    is_kind = (lane_out == 2 * TAIL + 4) | (lane_out == 2 * TAIL + 5)
    first = jnp.concatenate([got[:, 0:128], tails], axis=1)
    second = jnp.concatenate([got[:, 128:256], tails], axis=1)
    for start in range(0, slots, chunk):
        target = (iota((chunk, sources), 0) + start) * TILE
        heads, total = [], None
        for place in range(TILE):
            pick_low = jnp.where(target + place == low, 1.0, 0.0).astype(BF16)
            pick_high = jnp.where(target + place == high, 1.0, 0.0).astype(BF16)
            from_low = dot(pick_low, first)
            from_high = dot(pick_high, second)
            heads.append(from_low[:, 0:128] + from_high[:, 0:128])
            low_tail, high_tail = from_low[:, 128:256], from_high[:, 128:256]
            tail = low_tail + pltpu.roll(high_tail, 128 - TAIL, 1)
            kind = low_tail + pltpu.roll(high_tail, 126, 1)
            tail = jnp.where(lane_out < TAIL, tail, 0.0)
            kind = jnp.where(is_kind, kind, 0.0)
            if place:
                tail = pltpu.roll(tail, TAIL, 1)
                kind = pltpu.roll(kind, 2, 1)
            total = tail + kind if total is None else total + tail + kind
        out = out_ref.at[start // CAP : (start + chunk) // CAP]
        blocks = chunk // CAP
        out[:, :, 0:128] = heads[0].reshape(blocks, CAP, 128).astype(BF16)
        out[:, :, 128:256] = heads[1].reshape(blocks, CAP, 128).astype(BF16)
        out[:, :, 256:384] = total.reshape(blocks, CAP, 128).astype(BF16)


def route(got):
    bands = got.shape[0]
    return pl.pallas_call(
        route_kernel,
        in_specs=[VMEM],
        out_specs=VMEM,
        out_shape=jax.ShapeDtypeStruct((bands, CAP, 384), BF16),
        cost_estimate=pl.CostEstimate(
            flops=1_200_000_000, bytes_accessed=1_200_000, transcendentals=0
        ),
        name="route",
    )(got)


def work_kernel(got_ref, bias_ref, gain_ref, wqv_ref, wk_ref, proj_ref, out_ref, held, done):
    for part in range(held.shape[0]):
        values = got_ref[:, :, part * 128 : (part + 1) * 128].astype(F32)
        held[part] = values.reshape(TOKENS * CAP, 128)
    pairs = 2

    def two_slots(step, carry):
        tokens, masks = [], []
        for index in range(pairs):
            slot = step * pairs + index
            rows = pl.ds(slot, TOKENS, stride=CAP)
            tail = held[TILE, rows, :]
            for place in range(TILE):
                head = held[place, rows, :]
                moved = pltpu.roll(tail, 128 - TAIL, 1) if place else tail
                tokens.append(jnp.concatenate([head, moved], axis=1)[:, :CHAN])
            lane = iota((1, 128), 1) - 2 * TAIL - 4
            flags = [
                jnp.sum(jnp.where(lane == i, tail[0:1], 0.0), axis=1, keepdims=True)
                for i in range(4)
            ]
            masks.append(region_mask(flags[0::2], flags[1::2]))
        x = jnp.concatenate(tokens, axis=0)
        mixed = attend(x, masks, bias_ref, gain_ref[...], wqv_ref, wk_ref)
        for index in range(pairs):
            rows = pl.ds(step * pairs + index, CHAN, stride=CAP)
            own = x[index * PAIR : (index + 1) * PAIR]
            done[rows, :] = own.T + dot(proj_ref[...], mixed[index])
        return carry

    lax.fori_loop(0, CAP // pairs, two_slots, 0)
    out_ref[...] = done[...].reshape(CHAN, CAP, PAIR).astype(BF16)


def work_path(got, bias, gain, wqv, wk, proj):
    return pl.pallas_call(
        work_kernel,
        in_specs=[VMEM] * 6,
        out_specs=VMEM,
        out_shape=jax.ShapeDtypeStruct((CHAN, CAP, PAIR), BF16),
        scratch_shapes=[
            pltpu.VMEM((TILE + 1, TOKENS * CAP, 128), F32),
            pltpu.VMEM((CHAN * CAP, PAIR), F32),
        ],
        cost_estimate=pl.CostEstimate(
            flops=8_000_000_000, bytes_accessed=2_000_000, transcendentals=1_000_000
        ),
        name="work_path",
    )(got, bias, gain, wqv, wk, proj)


def from_behind(value, axis, steps):
    count = lax.axis_size(axis)
    pairs = [(source, (source + steps) % count) for source in range(count)]
    return lax.ppermute(value, axis, pairs)


def shards(
    pixels,
    keep_mask,
    band_counts,
    plan_dest,
    plan_slot,
    bias_table,
    gain_attn,
    qkv_weight,
    proj_weight,
    gain_mlp,
    hidden_weight,
    output_weight,
):
    gain_attn, gain_mlp = gain_attn[None], gain_mlp[None]
    pixels = jnp.transpose(pixels, (2, 0, 1))
    halo = from_behind(pixels[:, :SHIFT], "band", -1)
    outgoing, rest = spread(keep_mask, band_counts, plan_dest, plan_slot, pixels)
    gathered = lax.all_to_all(outgoing, "band", split_axis=0, concat_axis=0, tiled=True)
    wqv, wk, proj, proj_turned, bias = prep(qkv_weight, proj_weight, bias_table.T)
    finished = own_path(
        keep_mask,
        band_counts,
        rest,
        halo,
        bias,
        gain_attn,
        wqv,
        wk,
        proj,
        gain_mlp,
        hidden_weight,
        output_weight.T,
    )
    upper = from_behind(finished[:, :SHIFT], "band", 1)
    routed = route(gathered)
    incoming = lax.all_to_all(routed, "band", split_axis=0, concat_axis=0, tiled=True)
    restored = jnp.concatenate([upper, finished[:, SHIFT:]], axis=1)
    restored = jnp.transpose(restored, (1, 2, 0))
    work_tiles = work_path(incoming, bias, gain_attn, wqv, wk, proj_turned)
    work_tiles = jnp.transpose(work_tiles, (1, 2, 0))
    return (restored, work_tiles)


def solution(mesh):
    in_specs = (
        P(("img", "band"), None, None),
        P(("img", "band"), None),
        P(("img", "band")),
        P(("img", "band"), None),
        P(("img", "band"), None),
        P(),
        P(),
        P(),
        P(),
        P(),
        P(),
        P(),
    )
    out_specs = (P(("img", "band"), None, None), P(("img", "band"), None, None))
    return jax.shard_map(shards, mesh=mesh, in_specs=in_specs, out_specs=out_specs, check_vma=False)
```

```python
import jax
import jax.numpy as jnp
from jax import lax
from jax.experimental import pallas as pl
from jax.experimental.pallas import tpu as pltpu
from jax.sharding import PartitionSpec as P


CHAN = 180
HEADS = 6
HEAD_DIM = CHAN // HEADS
HEAD_PAD = 32
WIN = 8
TOKENS = WIN * WIN
TILE = 2
PAIR = TILE * TOKENS
SHIFT = 4
CAP = 8
TAIL = CHAN - 128
EPSILON = 1e-05

F32 = jnp.float32
BF16 = jnp.bfloat16


def dot(left, right, left_dim=1, right_dim=0):
    return lax.dot_general(
        left,
        right,
        (((left_dim,), (right_dim,)), ((), ())),
        preferred_element_type=F32,
    )


def layer_norm(values, gain):
    center = values - jnp.sum(values, axis=-1, keepdims=True) * (1.0 / CHAN)
    spread = jnp.sum(center * center, axis=-1, keepdims=True) * (1.0 / CHAN)
    return center * lax.rsqrt(spread + EPSILON) * gain


def iota(shape, dim):
    return lax.broadcasted_iota(jnp.int32, shape, dim)


def region_mask(row_flags, col_flags):
    shape = (TOKENS, PAIR)
    key, lane = iota(shape, 0), iota(shape, 1)
    first = lane < TOKENS
    row_differs = (((key >> 5) & 1) != ((lane >> 5) & 1)).astype(F32)
    col_differs = (((key >> 2) & 1) != ((lane >> 2) & 1)).astype(F32)
    row_on = jnp.where(first, row_flags[0], row_flags[1])
    col_on = jnp.where(first, col_flags[0], col_flags[1])
    return -100.0 * jnp.maximum(row_differs * row_on, col_differs * col_on)


def attend(x, masks, bias_ref, gain, wqv_ref, wk_ref):
    pairs = len(masks)
    normed = layer_norm(x, gain).astype(BF16)
    qv = dot(wqv_ref[...], normed, 1, 1)
    keys = dot(normed, wk_ref[...])
    key_low = (iota(keys.shape, 1) & 64) != 0
    keys = (keys - jnp.where(key_low, keys.astype(BF16).astype(F32), 0.0)).astype(BF16)
    half = HEADS * HEAD_PAD
    queries = qv[:half] * (HEAD_DIM ** (-0.5))
    high = queries.astype(BF16)
    low = (queries - high.astype(F32)).astype(BF16)
    values = qv[half:].astype(BF16)
    first_lane = iota((TOKENS, PAIR), 1) < TOKENS
    blank = jnp.zeros((PAIR, PAIR), BF16)
    scores = []
    for pair in range(pairs):
        lanes = slice(pair * PAIR, (pair + 1) * PAIR)
        for head in range(0, HEADS, 2):
            fours = []
            for one in (head, head + 1):
                rows = slice(one * HEAD_PAD, (one + 1) * HEAD_PAD)
                h, l = high[rows, lanes], low[rows, lanes]
                fours.append(jnp.concatenate([h, l, h, l], axis=0))
            both = jnp.concatenate(
                [
                    jnp.concatenate([fours[0], blank], axis=1),
                    jnp.concatenate([blank, fours[1]], axis=1),
                ],
                axis=0,
            )
            got = dot(keys[lanes, head * PAIR : (head + 2) * PAIR], both)
            for one in range(2):
                part = got[:, one * PAIR : (one + 1) * PAIR]
                scores.append(jnp.where(first_lane, part[:TOKENS], part[TOKENS:]))
    weights = []
    for pair in range(pairs):
        for head in range(HEADS):
            value = scores[pair * HEADS + head] + bias_ref[head] + masks[pair]
            value = jnp.exp(value - jnp.max(value, axis=0, keepdims=True))
            value = value * (1.0 / jnp.sum(value, axis=0, keepdims=True))
            weights.append(
                jnp.concatenate(
                    [jnp.where(first_lane, value, 0.0), jnp.where(first_lane, 0.0, value)], axis=0
                ).astype(BF16)
            )
    mixed = []
    for pair in range(pairs):
        lanes = slice(pair * PAIR, (pair + 1) * PAIR)
        parts = []
        for head in range(0, HEADS, 2):
            at = pair * HEADS + head
            both = jnp.concatenate([weights[at], weights[at + 1]], axis=1)
            rows = slice(head * HEAD_PAD, (head + 2) * HEAD_PAD)
            got = dot(values[rows, lanes], both)
            parts += [got[:HEAD_PAD, :PAIR], got[HEAD_PAD:, PAIR:]]
        mixed.append(jnp.concatenate(parts, axis=0).astype(BF16))
    return mixed


def feed(states, gain, hidden_ref, output_ref):
    normed = layer_norm(states, gain).astype(BF16)
    inner = jax.nn.gelu(dot(normed, hidden_ref[...]), approximate=True).astype(BF16)
    return states + dot(inner, output_ref[...], 1, 1)


def in_vmem(value):
    return pltpu.with_memory_space_constraint(value, pltpu.VMEM)


VMEM = pl.BlockSpec(memory_space=pltpu.VMEM)
SMEM = pl.BlockSpec(memory_space=pltpu.SMEM)


def pad_weights(qkv_ref, proj_ref, wqv_ref, wk_ref, padded_ref, turned_ref):
    half = HEADS * HEAD_PAD

    def source(column):
        inner = column & (HEAD_PAD - 1)
        return jnp.where(inner < HEAD_DIM, (column >> 5) * HEAD_DIM + inner, -1000)

    qkv = qkv_ref[...]
    column = iota((2 * half, 3 * CHAN), 0)
    wanted = jnp.where(column < half, source(column), 2 * CHAN + source(column - half))
    pick = (wanted == iota((2 * half, 3 * CHAN), 1)).astype(F32).astype(BF16)
    wqv_ref[...] = dot(pick, qkv, 1, 1).astype(BF16)
    shape = (3 * CHAN, HEADS * PAIR)
    column = iota(shape, 1)
    inner = column & (HEAD_PAD - 1)
    wanted = jnp.where(inner < HEAD_DIM, CHAN + (column >> 7) * HEAD_DIM + inner, -1)
    wk_ref[...] = dot(qkv, (wanted == iota(shape, 0)).astype(F32).astype(BF16)).astype(BF16)
    proj = proj_ref[...]
    pick = (source(iota((half, CHAN), 0)) == iota((half, CHAN), 1)).astype(F32).astype(BF16)
    padded_ref[...] = dot(pick, proj).astype(BF16)
    pick = (source(iota((CHAN, half), 1)) == iota((CHAN, half), 0)).astype(F32).astype(BF16)
    turned_ref[...] = dot(proj, pick, 0, 0).astype(BF16)


def spread_bias(table_ref, bias_ref, padded, looked):
    reach = 2 * WIN - 1
    padded[...] = jnp.zeros(padded.shape, F32)
    padded[0:HEADS, 0 : reach * reach] = table_ref[...]
    table = padded[...]
    for key in range(TOKENS):
        shift = 112 - (key // WIN) * reach - key % WIN
        moved = pltpu.roll(table, (256 - shift) % 256, 1)[:, :PAIR]
        looked[key * 8 : (key + 1) * 8, :] = moved
    rest = looked[...]
    query = iota((PAIR, PAIR), 1) & (TOKENS - 1)
    pick = (iota((PAIR, PAIR), 0) == (query >> 3) * reach + (query & 7)).astype(F32).astype(BF16)
    total = None
    for _ in range(3):
        part = rest.astype(BF16)
        rest = rest - part.astype(F32)
        got = dot(part, pick)
        total = got if total is None else total + got
    looked[...] = total
    for head in range(HEADS):
        bias_ref[head] = looked[pl.ds(head, TOKENS, stride=8), :]


def turned_rows(flat, row, stride):
    rows = pl.ds(row, 256, stride=stride)
    return jnp.concatenate([half[rows, :] for half in flat], axis=1).astype(BF16)


def hold_channels(block_ref, flat):
    channels, rows, _ = block_ref.shape
    for index, half in enumerate(flat):
        values = block_ref[:, :, index * 128 : (index + 1) * 128].astype(F32)
        half[0 : channels * rows, :] = values.reshape(channels * rows, 128)
        half[channels * rows :, :] = jnp.zeros((half.shape[0] - channels * rows, 128), F32)


def roll_pick(columns):
    wanted = (iota((columns, columns), 0) + SHIFT) & (columns - 1)
    return (wanted == iota((columns, columns), 1)).astype(F32).astype(BF16)


def own_kernel(
    keep_ref,
    count_ref,
    rest_ref,
    halo_ref,
    table_ref,
    qkv_ref,
    proj_ref,
    gain_attn_ref,
    gain_mlp_ref,
    hidden_ref,
    output_ref,
    sent_ref,
    kept_ref,
    wqv_ref,
    wk_ref,
    turned_ref,
    bias_ref,
    active,
    padded_proj,
    padded_table,
    looked,
    flat0,
    flat1,
    lower_rows,
    finished,
):
    columns_all = rest_ref.shape[1]
    pairs = 8
    steps = columns_all // (pairs * TILE * WIN)
    row_flag = jnp.where(lax.axis_index("band") == lax.axis_size("band") - 1, 1.0, 0.0)

    position = jnp.int32(-1)
    for w in range(keep_ref.shape[1]):
        keep = keep_ref[0, w]
        position = position + keep
        active[w] = jnp.where((keep == 1) & (position < count_ref[0]), 1, 0)
    pad_weights(qkv_ref, proj_ref, wqv_ref, wk_ref, padded_proj, turned_ref)
    spread_bias(table_ref, bias_ref, padded_table, looked)
    hold_channels(halo_ref, (flat0, flat1))
    pick = roll_pick(columns_all)
    for row in range(SHIFT):
        got = dot(pick, turned_rows((flat0, flat1), row, SHIFT), 1, 1)
        lower_rows[row] = got[:, :CHAN]

    def some_pairs(step, carry):
        tokens, masks = [], []
        for pair in range(pairs):
            start = pl.multiple_of((step * pairs + pair) * TILE * WIN, TILE * WIN)
            columns = pl.ds(start, TILE * WIN)
            upper = rest_ref[:, columns, :].astype(F32)
            lower = lower_rows[:, columns, :]
            for w in range(TILE):
                for part in (upper, lower):
                    tokens.append(
                        part[:, w * WIN : (w + 1) * WIN].reshape(SHIFT * WIN, CHAN)
                    )
            at_end = jnp.where((step == steps - 1) & (pair == pairs - 1), 1.0, 0.0)
            masks.append(region_mask((row_flag, row_flag), (0.0, at_end)))
        x = jnp.concatenate(tokens, axis=0)
        mixed = attend(x, masks, bias_ref, gain_attn_ref[...], wqv_ref, wk_ref)
        projected = [dot(part, padded_proj[...], 0, 0) for part in mixed]
        attended = x + jnp.concatenate(projected, axis=0)
        attended = attended.astype(BF16).astype(F32)
        done = feed(attended, gain_mlp_ref[...], hidden_ref, output_ref)
        for pair in range(pairs):
            start = pl.multiple_of((step * pairs + pair) * TILE * WIN, TILE * WIN)
            kept = []
            for w in range(TILE):
                at = pair * TILE + w
                on = active[step * pairs * TILE + at]
                rows = slice(at * TOKENS, (at + 1) * TOKENS)
                kept.append(jnp.where(on == 1, done[rows], x[rows]).reshape(WIN, WIN, CHAN))
            kept = jnp.concatenate(kept, axis=1).astype(BF16)
            finished[:, pl.ds(start, TILE * WIN), :] = kept
        return carry

    lax.fori_loop(0, steps, some_pairs, 0)

    same = (iota((CHAN, CHAN), 0) == iota((CHAN, CHAN), 1)).astype(F32).astype(BF16)
    for first, out_ref in ((0, kept_ref), (SHIFT, sent_ref)):
        for row in range(SHIFT):
            got = pltpu.roll(dot(same, finished[first + row], 1, 1), SHIFT, 1)
            rows = pl.ds(row, CHAN, stride=SHIFT)
            flat0[rows, :] = got[:, :128]
            flat1[rows, :] = got[:, 128:]
        for index, flat in enumerate((flat0, flat1)):
            values = flat[0 : CHAN * SHIFT, :].reshape(CHAN, SHIFT, 128)
            out_ref[:, :, index * 128 : (index + 1) * 128] = values.astype(BF16)


def own_path(keep, count, rest, halo, table, qkv, proj, gain_attn, gain_mlp, hidden, output):
    _, columns, _ = rest.shape
    half = HEADS * HEAD_PAD
    flat = pltpu.VMEM((256 * SHIFT, 128), F32)
    part = jax.ShapeDtypeStruct((CHAN, SHIFT, columns), BF16)
    return pl.pallas_call(
        own_kernel,
        in_specs=[SMEM, SMEM] + [VMEM] * 9,
        out_specs=[VMEM] * 6,
        out_shape=[
            part,
            part,
            jax.ShapeDtypeStruct((2 * half, CHAN), BF16),
            jax.ShapeDtypeStruct((CHAN, HEADS * PAIR), BF16),
            jax.ShapeDtypeStruct((CHAN, half), BF16),
            jax.ShapeDtypeStruct((HEADS, TOKENS, PAIR), F32),
        ],
        scratch_shapes=[
            pltpu.SMEM((columns // WIN,), jnp.int32),
            pltpu.VMEM((half, CHAN), BF16),
            pltpu.VMEM((8, 256), F32),
            pltpu.VMEM((8 * TOKENS, PAIR), F32),
            flat,
            flat,
            pltpu.VMEM((SHIFT, columns, CHAN), F32),
            pltpu.VMEM((WIN, columns, CHAN), BF16),
        ],
        cost_estimate=pl.CostEstimate(
            flops=20_000_000_000, bytes_accessed=3_000_000, transcendentals=2_000_000
        ),
        name="own_path",
    )(keep, count, rest, in_vmem(halo), table, qkv, proj, gain_attn, gain_mlp, hidden, output)


def spread_kernel(
    keep_ref, count_ref, dest_ref, slot_ref, pixels_ref, out_ref, rest_ref, flat0, flat1
):
    _, rows, columns = pixels_ref.shape
    windows = columns // WIN
    half = windows // 2
    bands = lax.axis_size("band")
    last_band = jnp.where(lax.axis_index("band") == bands - 1, 1.0, 0.0)
    row, lane = iota((half, 128), 0), iota((half, 128), 1) - 2 * TAIL
    codes = jnp.where((lane == 4) | (lane == 6), last_band, 0.0)
    codes = jnp.where((lane == 7) & (row == half - 1), 1.0, codes)
    position = jnp.int32(-1)
    for w in range(windows):
        keep = keep_ref[0, w]
        position = position + keep
        tile = jnp.maximum(position, 0) >> 1
        slot = slot_ref[0, tile]
        placed = (keep == 1) & (position < count_ref[0]) & (slot < CAP)
        dest = jnp.where(placed, dest_ref[0, tile], bands).astype(F32)
        place = jnp.where(placed, slot * TILE + (position & 1), 0).astype(F32)
        first = 2 * (w // half)
        here = row == w % half
        codes = jnp.where(here & (lane == first), dest, codes)
        codes = jnp.where(here & (lane == first + 1), place, codes)

    hold_channels(pixels_ref, (flat0, flat1))
    out_row = iota((columns, columns), 0)
    wanted = ((out_row & (windows - 1)) * WIN + (out_row >> 5) + SHIFT) & (columns - 1)
    group = (wanted == iota((columns, columns), 1)).astype(F32).astype(BF16)
    pick = roll_pick(columns)
    for r in range(rows):
        line = turned_rows((flat0, flat1), r, rows)
        if r >= SHIFT:
            rest_ref[r - SHIFT] = dot(pick, line, 1, 1)[:, :CHAN].astype(BF16)
        got = dot(group, line, 1, 1)
        for cu in range(WIN):
            token = (r + SHIFT) % rows * WIN + cu
            low = got[cu * windows : cu * windows + half]
            high = got[cu * windows + half : (cu + 1) * windows]
            packed = low[:, 128:] + pltpu.roll(high[:, 128:], TAIL, 1) + codes
            out_ref[token, :, 0:128] = low[:, :128].astype(BF16)
            out_ref[token, :, 128:256] = high[:, :128].astype(BF16)
            out_ref[token, :, 256:384] = packed.astype(BF16)


def spread(keep, count, dest, slot, pixels):
    _, rows, columns = pixels.shape
    half = columns // WIN // 2
    flat = pltpu.VMEM((256 * rows, 128), F32)
    return pl.pallas_call(
        spread_kernel,
        in_specs=[SMEM] * 4 + [VMEM],
        out_specs=[VMEM] * 2,
        out_shape=[
            jax.ShapeDtypeStruct((TOKENS, half, 384), BF16),
            jax.ShapeDtypeStruct((SHIFT, columns, CHAN), BF16),
        ],
        scratch_shapes=[flat, flat],
        cost_estimate=pl.CostEstimate(
            flops=500_000_000, bytes_accessed=2_000_000, transcendentals=0
        ),
        name="spread",
    )(keep, count, dest, slot, pixels)


def route_kernel(got_ref, out_ref):
    bands, half, _ = got_ref.shape
    slots = out_ref.shape[0] * out_ref.shape[1]
    sources = bands * half
    got = got_ref[...].reshape(sources, 384)
    tails = got[:, 256:384]
    row = iota((8, 128), 0)
    lane = iota((8, 128), 1) - 2 * TAIL - 2 * row
    pick = jnp.where(row < 2, jnp.where(lane == 0, 16.0, jnp.where(lane == 1, 1.0, 0.0)), 0.0)
    codes = dot(pick.astype(BF16), tails, 1, 1)
    behind = lax.axis_index("band") >= TOKENS // 2
    codes = jnp.where(behind, pltpu.roll(codes, half, 1), codes)
    low, high = codes[0:1].astype(jnp.int32), codes[1:2].astype(jnp.int32)
    chunk = 256
    lane_out = iota((chunk, 128), 1)
    is_kind = (lane_out == 2 * TAIL + 4) | (lane_out == 2 * TAIL + 5)
    first = jnp.concatenate([got[:, 0:128], tails], axis=1)
    second = jnp.concatenate([got[:, 128:256], tails], axis=1)
    for start in range(0, slots, chunk):
        target = (iota((chunk, sources), 0) + start) * TILE
        heads, total = [], None
        for place in range(TILE):
            pick_low = jnp.where(target + place == low, 1.0, 0.0).astype(BF16)
            pick_high = jnp.where(target + place == high, 1.0, 0.0).astype(BF16)
            from_low = dot(pick_low, first)
            from_high = dot(pick_high, second)
            heads.append(from_low[:, 0:128] + from_high[:, 0:128])
            low_tail, high_tail = from_low[:, 128:256], from_high[:, 128:256]
            tail = low_tail + pltpu.roll(high_tail, 128 - TAIL, 1)
            kind = low_tail + pltpu.roll(high_tail, 126, 1)
            tail = jnp.where(lane_out < TAIL, tail, 0.0)
            kind = jnp.where(is_kind, kind, 0.0)
            if place:
                tail = pltpu.roll(tail, TAIL, 1)
                kind = pltpu.roll(kind, 2, 1)
            total = tail + kind if total is None else total + tail + kind
        out = out_ref.at[start // CAP : (start + chunk) // CAP]
        blocks = chunk // CAP
        out[:, :, 0:128] = heads[0].reshape(blocks, CAP, 128).astype(BF16)
        out[:, :, 128:256] = heads[1].reshape(blocks, CAP, 128).astype(BF16)
        out[:, :, 256:384] = total.reshape(blocks, CAP, 128).astype(BF16)


def route(got):
    bands = got.shape[0]
    return pl.pallas_call(
        route_kernel,
        in_specs=[VMEM],
        out_specs=VMEM,
        out_shape=jax.ShapeDtypeStruct((bands, CAP, 384), BF16),
        cost_estimate=pl.CostEstimate(
            flops=1_200_000_000, bytes_accessed=1_200_000, transcendentals=0
        ),
        name="route",
    )(in_vmem(got))


def work_kernel(got_ref, bias_ref, gain_ref, wqv_ref, wk_ref, proj_ref, out_ref, held, done):
    for part in range(held.shape[0]):
        values = got_ref[:, :, part * 128 : (part + 1) * 128].astype(F32)
        held[part] = values.reshape(TOKENS * CAP, 128)
    pairs = 8

    def some_slots(step, carry):
        tokens, masks = [], []
        for index in range(pairs):
            slot = step * pairs + index
            rows = pl.ds(slot, TOKENS, stride=CAP)
            tail = held[TILE, rows, :]
            for place in range(TILE):
                head = held[place, rows, :]
                moved = pltpu.roll(tail, 128 - TAIL, 1) if place else tail
                tokens.append(jnp.concatenate([head, moved], axis=1)[:, :CHAN])
            lane = iota((1, 128), 1) - 2 * TAIL - 4
            flags = [
                jnp.sum(jnp.where(lane == i, tail[0:1], 0.0), axis=1, keepdims=True)
                for i in range(4)
            ]
            masks.append(region_mask(flags[0::2], flags[1::2]))
        x = jnp.concatenate(tokens, axis=0)
        mixed = attend(x, masks, bias_ref, gain_ref[...], wqv_ref, wk_ref)
        for index in range(pairs):
            rows = pl.ds(step * pairs + index, CHAN, stride=CAP)
            own = x[index * PAIR : (index + 1) * PAIR]
            done[rows, :] = own.T + dot(proj_ref[...], mixed[index])
        return carry

    lax.fori_loop(0, CAP // pairs, some_slots, 0)
    out_ref[...] = done[...].reshape(CHAN, CAP, PAIR).astype(BF16)


def work_path(got, bias, gain, wqv, wk, proj):
    return pl.pallas_call(
        work_kernel,
        in_specs=[VMEM] * 6,
        out_specs=VMEM,
        out_shape=jax.ShapeDtypeStruct((CHAN, CAP, PAIR), BF16),
        scratch_shapes=[
            pltpu.VMEM((TILE + 1, TOKENS * CAP, 128), F32),
            pltpu.VMEM((CHAN * CAP, PAIR), F32),
        ],
        cost_estimate=pl.CostEstimate(
            flops=8_000_000_000, bytes_accessed=2_000_000, transcendentals=1_000_000
        ),
        name="work_path",
    )(in_vmem(got), bias, gain, wqv, wk, proj)


def from_behind(value, axis, steps):
    count = lax.axis_size(axis)
    pairs = [(source, (source + steps) % count) for source in range(count)]
    return lax.ppermute(value, axis, pairs)


def shards(
    pixels,
    keep_mask,
    band_counts,
    plan_dest,
    plan_slot,
    bias_table,
    gain_attn,
    qkv_weight,
    proj_weight,
    gain_mlp,
    hidden_weight,
    output_weight,
):
    gain_attn, gain_mlp = gain_attn[None], gain_mlp[None]
    pixels = jnp.transpose(pixels, (2, 0, 1))
    halo = from_behind(pixels[:, :SHIFT], "band", -1)
    outgoing, rest = spread(keep_mask, band_counts, plan_dest, plan_slot, pixels)
    gathered = lax.all_to_all(outgoing, "band", split_axis=0, concat_axis=0, tiled=True)
    sent, kept, wqv, wk, proj, bias = own_path(
        keep_mask,
        band_counts,
        rest,
        halo,
        bias_table.T,
        qkv_weight,
        proj_weight,
        gain_attn,
        gain_mlp,
        hidden_weight,
        output_weight.T,
    )
    upper = from_behind(sent, "band", 1)
    routed = route(gathered)
    incoming = lax.all_to_all(routed, "band", split_axis=0, concat_axis=0, tiled=True)
    restored = jnp.concatenate([upper, kept], axis=1)
    restored = jnp.transpose(restored, (1, 2, 0))
    work_tiles = work_path(incoming, bias, gain_attn, wqv, wk, proj)
    work_tiles = jnp.transpose(work_tiles, (1, 2, 0))
    return (restored, work_tiles)


def solution(mesh):
    in_specs = (
        P(("img", "band"), None, None),
        P(("img", "band"), None),
        P(("img", "band")),
        P(("img", "band"), None),
        P(("img", "band"), None),
        P(),
        P(),
        P(),
        P(),
        P(),
        P(),
        P(),
    )
    out_specs = (P(("img", "band"), None, None), P(("img", "band"), None, None))
    return jax.shard_map(shards, mesh=mesh, in_specs=in_specs, out_specs=out_specs, check_vma=False)
```

```python
import jax
import jax.numpy as jnp
from jax import lax
from jax.experimental import pallas as pl
from jax.experimental.pallas import tpu as pltpu
from jax.sharding import PartitionSpec as P


CHAN = 180
HEADS = 6
HEAD_DIM = CHAN // HEADS
HEAD_PAD = 32
WIN = 8
TOKENS = WIN * WIN
TILE = 2
PAIR = TILE * TOKENS
SHIFT = 4
CAP = 8
TAIL = CHAN - 128
EPSILON = 1e-05

F32 = jnp.float32
BF16 = jnp.bfloat16


def dot(left, right, left_dim=1, right_dim=0):
    return lax.dot_general(
        left,
        right,
        (((left_dim,), (right_dim,)), ((), ())),
        preferred_element_type=F32,
    )


def layer_norm(values, gain):
    center = values - jnp.sum(values, axis=-1, keepdims=True) * (1.0 / CHAN)
    spread = jnp.sum(center * center, axis=-1, keepdims=True) * (1.0 / CHAN)
    return center * lax.rsqrt(spread + EPSILON) * gain


def iota(shape, dim):
    return lax.broadcasted_iota(jnp.int32, shape, dim)


def region_mask(row_flags, col_flags):
    shape = (TOKENS, PAIR)
    key, lane = iota(shape, 0), iota(shape, 1)
    first = lane < TOKENS
    row_differs = (((key >> 5) & 1) != ((lane >> 5) & 1)).astype(F32)
    col_differs = (((key >> 2) & 1) != ((lane >> 2) & 1)).astype(F32)
    row_on = jnp.where(first, row_flags[0], row_flags[1])
    col_on = jnp.where(first, col_flags[0], col_flags[1])
    return -100.0 * jnp.maximum(row_differs * row_on, col_differs * col_on)


def attend(x, masks, bias_ref, gain, wqv_ref, wk_ref):
    pairs = len(masks)
    normed = layer_norm(x, gain).astype(BF16)
    qv = dot(wqv_ref[...], normed, 1, 1)
    keys = dot(normed, wk_ref[...])
    key_low = (iota(keys.shape, 1) & 64) != 0
    keys = (keys - jnp.where(key_low, keys.astype(BF16).astype(F32), 0.0)).astype(BF16)
    half = HEADS * HEAD_PAD
    queries = qv[:half] * (HEAD_DIM ** (-0.5))
    high = queries.astype(BF16)
    low = (queries - high.astype(F32)).astype(BF16)
    values = qv[half:].astype(BF16)
    first_lane = iota((TOKENS, PAIR), 1) < TOKENS
    blank = jnp.zeros((PAIR, PAIR), BF16)
    scores = []
    for pair in range(pairs):
        lanes = slice(pair * PAIR, (pair + 1) * PAIR)
        for head in range(0, HEADS, 2):
            fours = []
            for one in (head, head + 1):
                rows = slice(one * HEAD_PAD, (one + 1) * HEAD_PAD)
                h, l = high[rows, lanes], low[rows, lanes]
                fours.append(jnp.concatenate([h, l, h, l], axis=0))
            both = jnp.concatenate(
                [
                    jnp.concatenate([fours[0], blank], axis=1),
                    jnp.concatenate([blank, fours[1]], axis=1),
                ],
                axis=0,
            )
            got = dot(keys[lanes, head * PAIR : (head + 2) * PAIR], both)
            for one in range(2):
                part = got[:, one * PAIR : (one + 1) * PAIR]
                scores.append(jnp.where(first_lane, part[:TOKENS], part[TOKENS:]))
    weights = []
    for pair in range(pairs):
        for head in range(HEADS):
            value = scores[pair * HEADS + head] + bias_ref[head] + masks[pair]
            value = jnp.exp(value - jnp.max(value, axis=0, keepdims=True))
            value = value * (1.0 / jnp.sum(value, axis=0, keepdims=True))
            weights.append(
                jnp.concatenate(
                    [jnp.where(first_lane, value, 0.0), jnp.where(first_lane, 0.0, value)], axis=0
                ).astype(BF16)
            )
    mixed = []
    for pair in range(pairs):
        lanes = slice(pair * PAIR, (pair + 1) * PAIR)
        parts = []
        for head in range(0, HEADS, 2):
            at = pair * HEADS + head
            both = jnp.concatenate([weights[at], weights[at + 1]], axis=1)
            rows = slice(head * HEAD_PAD, (head + 2) * HEAD_PAD)
            got = dot(values[rows, lanes], both)
            parts += [got[:HEAD_PAD, :PAIR], got[HEAD_PAD:, PAIR:]]
        mixed.append(jnp.concatenate(parts, axis=0).astype(BF16))
    return mixed


def feed(states, gain, hidden_ref, output_ref):
    normed = layer_norm(states, gain).astype(BF16)
    inner = jax.nn.gelu(dot(normed, hidden_ref[...]), approximate=True).astype(BF16)
    return states + dot(inner, output_ref[...], 1, 1)


def in_vmem(value):
    return pltpu.with_memory_space_constraint(value, pltpu.VMEM)


VMEM = pl.BlockSpec(memory_space=pltpu.VMEM)
SMEM = pl.BlockSpec(memory_space=pltpu.SMEM)


def pad_weights(qkv_ref, proj_ref, wqv_ref, wk_ref, padded_ref, turned_ref):
    half = HEADS * HEAD_PAD

    def source(column):
        inner = column & (HEAD_PAD - 1)
        return jnp.where(inner < HEAD_DIM, (column >> 5) * HEAD_DIM + inner, -1000)

    qkv = qkv_ref[...]
    column = iota((2 * half, 3 * CHAN), 0)
    wanted = jnp.where(column < half, source(column), 2 * CHAN + source(column - half))
    pick = (wanted == iota((2 * half, 3 * CHAN), 1)).astype(F32).astype(BF16)
    wqv_ref[...] = dot(pick, qkv, 1, 1).astype(BF16)
    shape = (3 * CHAN, HEADS * PAIR)
    column = iota(shape, 1)
    inner = column & (HEAD_PAD - 1)
    wanted = jnp.where(inner < HEAD_DIM, CHAN + (column >> 7) * HEAD_DIM + inner, -1)
    wk_ref[...] = dot(qkv, (wanted == iota(shape, 0)).astype(F32).astype(BF16)).astype(BF16)
    proj = proj_ref[...]
    pick = (source(iota((half, CHAN), 0)) == iota((half, CHAN), 1)).astype(F32).astype(BF16)
    padded_ref[...] = dot(pick, proj).astype(BF16)
    pick = (source(iota((CHAN, half), 1)) == iota((CHAN, half), 0)).astype(F32).astype(BF16)
    turned_ref[...] = dot(proj, pick, 0, 0).astype(BF16)


def spread_bias(table_ref, bias_ref, padded, looked):
    reach = 2 * WIN - 1
    padded[...] = jnp.zeros(padded.shape, F32)
    padded[0:HEADS, 0 : reach * reach] = table_ref[...]
    table = padded[...]
    for key in range(TOKENS):
        shift = 112 - (key // WIN) * reach - key % WIN
        moved = pltpu.roll(table, (256 - shift) % 256, 1)[:, :PAIR]
        looked[key * 8 : (key + 1) * 8, :] = moved
    rest = looked[...]
    query = iota((PAIR, PAIR), 1) & (TOKENS - 1)
    pick = (iota((PAIR, PAIR), 0) == (query >> 3) * reach + (query & 7)).astype(F32).astype(BF16)
    total = None
    for _ in range(3):
        part = rest.astype(BF16)
        rest = rest - part.astype(F32)
        got = dot(part, pick)
        total = got if total is None else total + got
    looked[...] = total
    for head in range(HEADS):
        bias_ref[head] = looked[pl.ds(head, TOKENS, stride=8), :]


def turned_rows(flat, row, stride):
    rows = pl.ds(row, 256, stride=stride)
    return jnp.concatenate([half[rows, :] for half in flat], axis=1).astype(BF16)


def hold_channels(block_ref, flat):
    channels, rows, _ = block_ref.shape
    for index, half in enumerate(flat):
        values = block_ref[:, :, index * 128 : (index + 1) * 128].astype(F32)
        half[0 : channels * rows, :] = values.reshape(channels * rows, 128)
        half[channels * rows :, :] = jnp.zeros((half.shape[0] - channels * rows, 128), F32)


def roll_pick(columns):
    wanted = (iota((columns, columns), 0) + SHIFT) & (columns - 1)
    return (wanted == iota((columns, columns), 1)).astype(F32).astype(BF16)


def own_kernel(
    keep_ref,
    count_ref,
    pixels_ref,
    halo_ref,
    table_ref,
    qkv_ref,
    proj_ref,
    gain_attn_ref,
    gain_mlp_ref,
    hidden_ref,
    output_ref,
    sent_ref,
    kept_ref,
    wqv_ref,
    wk_ref,
    turned_ref,
    bias_ref,
    active,
    padded_proj,
    padded_table,
    looked,
    flat0,
    flat1,
    wide0,
    wide1,
    lower_rows,
    upper_rows,
    finished,
):
    columns_all = pixels_ref.shape[2]
    pairs = 8
    steps = columns_all // (pairs * TILE * WIN)
    row_flag = jnp.where(lax.axis_index("band") == lax.axis_size("band") - 1, 1.0, 0.0)

    position = jnp.int32(-1)
    for w in range(keep_ref.shape[1]):
        keep = keep_ref[0, w]
        position = position + keep
        active[w] = jnp.where((keep == 1) & (position < count_ref[0]), 1, 0)
    pad_weights(qkv_ref, proj_ref, wqv_ref, wk_ref, padded_proj, turned_ref)
    spread_bias(table_ref, bias_ref, padded_table, looked)
    hold_channels(halo_ref, (flat0, flat1))
    pick = roll_pick(columns_all)
    for row in range(SHIFT):
        got = dot(pick, turned_rows((flat0, flat1), row, SHIFT), 1, 1)
        lower_rows[row] = got[:, :CHAN]
    hold_channels(pixels_ref, (wide0, wide1))
    for row in range(SHIFT):
        got = dot(pick, turned_rows((wide0, wide1), SHIFT + row, WIN), 1, 1)
        upper_rows[row] = got[:, :CHAN]

    def some_pairs(step, carry):
        tokens, masks = [], []
        for pair in range(pairs):
            start = pl.multiple_of((step * pairs + pair) * TILE * WIN, TILE * WIN)
            columns = pl.ds(start, TILE * WIN)
            upper = upper_rows[:, columns, :]
            lower = lower_rows[:, columns, :]
            for w in range(TILE):
                for part in (upper, lower):
                    tokens.append(
                        part[:, w * WIN : (w + 1) * WIN].reshape(SHIFT * WIN, CHAN)
                    )
            at_end = jnp.where((step == steps - 1) & (pair == pairs - 1), 1.0, 0.0)
            masks.append(region_mask((row_flag, row_flag), (0.0, at_end)))
        x = jnp.concatenate(tokens, axis=0)
        mixed = attend(x, masks, bias_ref, gain_attn_ref[...], wqv_ref, wk_ref)
        projected = [dot(part, padded_proj[...], 0, 0) for part in mixed]
        attended = x + jnp.concatenate(projected, axis=0)
        attended = attended.astype(BF16).astype(F32)
        done = feed(attended, gain_mlp_ref[...], hidden_ref, output_ref)
        for pair in range(pairs):
            start = pl.multiple_of((step * pairs + pair) * TILE * WIN, TILE * WIN)
            kept = []
            for w in range(TILE):
                at = pair * TILE + w
                on = active[step * pairs * TILE + at]
                rows = slice(at * TOKENS, (at + 1) * TOKENS)
                kept.append(jnp.where(on == 1, done[rows], x[rows]).reshape(WIN, WIN, CHAN))
            kept = jnp.concatenate(kept, axis=1).astype(BF16)
            finished[:, pl.ds(start, TILE * WIN), :] = kept
        return carry

    lax.fori_loop(0, steps, some_pairs, 0)

    same = (iota((CHAN, CHAN), 0) == iota((CHAN, CHAN), 1)).astype(F32).astype(BF16)
    for first, out_ref in ((0, kept_ref), (SHIFT, sent_ref)):
        for row in range(SHIFT):
            got = pltpu.roll(dot(same, finished[first + row], 1, 1), SHIFT, 1)
            rows = pl.ds(row, CHAN, stride=SHIFT)
            flat0[rows, :] = got[:, :128]
            flat1[rows, :] = got[:, 128:]
        for index, flat in enumerate((flat0, flat1)):
            values = flat[0 : CHAN * SHIFT, :].reshape(CHAN, SHIFT, 128)
            out_ref[:, :, index * 128 : (index + 1) * 128] = values.astype(BF16)


def own_path(keep, count, pixels, halo, table, qkv, proj, gain_attn, gain_mlp, hidden, output):
    columns = pixels.shape[2]
    half = HEADS * HEAD_PAD
    flat = pltpu.VMEM((256 * SHIFT, 128), F32)
    wide = pltpu.VMEM((256 * WIN, 128), F32)
    rows = pltpu.VMEM((SHIFT, columns, CHAN), F32)
    part = jax.ShapeDtypeStruct((CHAN, SHIFT, columns), BF16)
    return pl.pallas_call(
        own_kernel,
        in_specs=[SMEM, SMEM] + [VMEM] * 9,
        out_specs=[VMEM] * 6,
        out_shape=[
            part,
            part,
            pltpu.VMEM((2 * half, CHAN), BF16),
            pltpu.VMEM((CHAN, HEADS * PAIR), BF16),
            pltpu.VMEM((CHAN, half), BF16),
            pltpu.VMEM((HEADS, TOKENS, PAIR), F32),
        ],
        scratch_shapes=[
            pltpu.SMEM((columns // WIN,), jnp.int32),
            pltpu.VMEM((half, CHAN), BF16),
            pltpu.VMEM((8, 256), F32),
            pltpu.VMEM((8 * TOKENS, PAIR), F32),
            flat,
            flat,
            wide,
            wide,
            rows,
            rows,
            pltpu.VMEM((WIN, columns, CHAN), BF16),
        ],
        cost_estimate=pl.CostEstimate(
            flops=20_000_000_000, bytes_accessed=3_000_000, transcendentals=2_000_000
        ),
        name="own_path",
    )(keep, count, pixels, in_vmem(halo), table, qkv, proj, gain_attn, gain_mlp, hidden, output)


def spread_kernel(
    keep_ref,
    count_ref,
    dest_ref,
    slot_ref,
    pixels_ref,
    out_ref,
    top_ref,
    flat0,
    flat1,
):
    _, rows, columns = pixels_ref.shape
    windows = columns // WIN
    half = windows // 2
    bands = lax.axis_size("band")
    last_band = jnp.where(lax.axis_index("band") == bands - 1, 1.0, 0.0)
    row, lane = iota((half, 128), 0), iota((half, 128), 1) - 2 * TAIL
    codes = jnp.where((lane == 4) | (lane == 6), last_band, 0.0)
    codes = jnp.where((lane == 7) & (row == half - 1), 1.0, codes)
    position = jnp.int32(-1)
    for w in range(windows):
        keep = keep_ref[0, w]
        position = position + keep
        tile = jnp.maximum(position, 0) >> 1
        slot = slot_ref[0, tile]
        placed = (keep == 1) & (position < count_ref[0]) & (slot < CAP)
        dest = jnp.where(placed, bands - 1 - dest_ref[0, tile], bands).astype(F32)
        place = jnp.where(placed, slot * TILE + (position & 1), 0).astype(F32)
        first = 2 * (w // half)
        here = row == w % half
        codes = jnp.where(here & (lane == first), dest, codes)
        codes = jnp.where(here & (lane == first + 1), place, codes)

    top_ref[...] = pixels_ref[:, 0:SHIFT, :]
    hold_channels(pixels_ref, (flat0, flat1))
    out_row = iota((columns, columns), 0)
    wanted = ((out_row & (windows - 1)) * WIN + (out_row >> 5) + SHIFT) & (columns - 1)
    group = (wanted == iota((columns, columns), 1)).astype(F32).astype(BF16)
    for r in range(rows):
        got = dot(group, turned_rows((flat0, flat1), r, rows), 1, 1)
        for cu in range(WIN):
            token = (r + SHIFT) % rows * WIN + cu
            low = got[cu * windows : cu * windows + half]
            high = got[cu * windows + half : (cu + 1) * windows]
            packed = low[:, 128:] + pltpu.roll(high[:, 128:], TAIL, 1) + codes
            out_ref[token, :, 0:128] = low[:, :128].astype(BF16)
            out_ref[token, :, 128:256] = high[:, :128].astype(BF16)
            out_ref[token, :, 256:384] = packed.astype(BF16)


def spread(keep, count, dest, slot, pixels):
    channels, rows, columns = pixels.shape
    half = columns // WIN // 2
    flat = pltpu.VMEM((256 * rows, 128), F32)
    return pl.pallas_call(
        spread_kernel,
        in_specs=[SMEM] * 4 + [VMEM],
        out_specs=[VMEM] * 2,
        out_shape=[
            jax.ShapeDtypeStruct((TOKENS, half, 384), BF16),
            jax.ShapeDtypeStruct((channels, SHIFT, columns), BF16),
        ],
        scratch_shapes=[flat, flat],
        cost_estimate=pl.CostEstimate(
            flops=500_000_000, bytes_accessed=2_000_000, transcendentals=0
        ),
        name="spread",
    )(keep, count, dest, slot, pixels)


def route_kernel(got_ref, out_ref):
    bands, half, _ = got_ref.shape
    slots = out_ref.shape[0] * out_ref.shape[1]
    sources = bands * half
    got = got_ref[...].reshape(sources, 384)
    tails = got[:, 256:384]
    row = iota((8, 128), 0)
    lane = iota((8, 128), 1) - 2 * TAIL - 2 * row
    pick = jnp.where(row < 2, jnp.where(lane == 0, 16.0, jnp.where(lane == 1, 1.0, 0.0)), 0.0)
    codes = dot(pick.astype(BF16), tails, 1, 1)
    behind = bands - 1 - lax.axis_index("band") >= TOKENS // 2
    codes = jnp.where(behind, pltpu.roll(codes, sources - half, 1), codes)
    low, high = codes[0:1].astype(jnp.int32), codes[1:2].astype(jnp.int32)
    chunk = 256
    lane_out = iota((chunk, 128), 1)
    is_kind = (lane_out == 2 * TAIL + 4) | (lane_out == 2 * TAIL + 5)
    first = jnp.concatenate([got[:, 0:128], tails], axis=1)
    second = jnp.concatenate([got[:, 128:256], tails], axis=1)
    for start in range(0, slots, chunk):
        target = (iota((chunk, sources), 0) + start) * TILE
        heads, total = [], None
        for place in range(TILE):
            pick_low = jnp.where(target + place == low, 1.0, 0.0).astype(BF16)
            pick_high = jnp.where(target + place == high, 1.0, 0.0).astype(BF16)
            from_low = dot(pick_low, first)
            from_high = dot(pick_high, second)
            heads.append(from_low[:, 0:128] + from_high[:, 0:128])
            low_tail, high_tail = from_low[:, 128:256], from_high[:, 128:256]
            tail = low_tail + pltpu.roll(high_tail, 128 - TAIL, 1)
            kind = low_tail + pltpu.roll(high_tail, 126, 1)
            tail = jnp.where(lane_out < TAIL, tail, 0.0)
            kind = jnp.where(is_kind, kind, 0.0)
            if place:
                tail = pltpu.roll(tail, TAIL, 1)
                kind = pltpu.roll(kind, 2, 1)
            total = tail + kind if total is None else total + tail + kind
        out = out_ref.at[start // CAP : (start + chunk) // CAP]
        blocks = chunk // CAP
        out[:, :, 0:128] = heads[0].reshape(blocks, CAP, 128).astype(BF16)
        out[:, :, 128:256] = heads[1].reshape(blocks, CAP, 128).astype(BF16)
        out[:, :, 256:384] = total.reshape(blocks, CAP, 128).astype(BF16)


def route(got):
    bands = got.shape[0]
    return pl.pallas_call(
        route_kernel,
        in_specs=[VMEM],
        out_specs=VMEM,
        out_shape=jax.ShapeDtypeStruct((bands, CAP, 384), BF16),
        cost_estimate=pl.CostEstimate(
            flops=1_200_000_000, bytes_accessed=1_200_000, transcendentals=0
        ),
        name="route",
    )(in_vmem(got))


def work_kernel(got_ref, bias_ref, gain_ref, wqv_ref, wk_ref, proj_ref, out_ref, held, done):
    for part in range(held.shape[0]):
        values = got_ref[:, :, part * 128 : (part + 1) * 128].astype(F32)
        held[part] = values.reshape(TOKENS * CAP, 128)
    pairs = 8

    def some_slots(step, carry):
        tokens, masks = [], []
        for index in range(pairs):
            slot = step * pairs + index
            rows = pl.ds(slot, TOKENS, stride=CAP)
            tail = held[TILE, rows, :]
            for place in range(TILE):
                head = held[place, rows, :]
                moved = pltpu.roll(tail, 128 - TAIL, 1) if place else tail
                tokens.append(jnp.concatenate([head, moved], axis=1)[:, :CHAN])
            lane = iota((1, 128), 1) - 2 * TAIL - 4
            flags = [
                jnp.sum(jnp.where(lane == i, tail[0:1], 0.0), axis=1, keepdims=True)
                for i in range(4)
            ]
            masks.append(region_mask(flags[0::2], flags[1::2]))
        x = jnp.concatenate(tokens, axis=0)
        mixed = attend(x, masks, bias_ref, gain_ref[...], wqv_ref, wk_ref)
        for index in range(pairs):
            rows = pl.ds(step * pairs + index, CHAN, stride=CAP)
            own = x[index * PAIR : (index + 1) * PAIR]
            done[rows, :] = own.T + dot(proj_ref[...], mixed[index])
        return carry

    lax.fori_loop(0, CAP // pairs, some_slots, 0)
    out_ref[...] = done[...].reshape(CHAN, CAP, PAIR).astype(BF16)


def work_path(got, bias, gain, wqv, wk, proj):
    return pl.pallas_call(
        work_kernel,
        in_specs=[VMEM] * 6,
        out_specs=VMEM,
        out_shape=jax.ShapeDtypeStruct((CHAN, CAP, PAIR), BF16),
        scratch_shapes=[
            pltpu.VMEM((TILE + 1, TOKENS * CAP, 128), F32),
            pltpu.VMEM((CHAN * CAP, PAIR), F32),
        ],
        cost_estimate=pl.CostEstimate(
            flops=8_000_000_000, bytes_accessed=2_000_000, transcendentals=1_000_000
        ),
        name="work_path",
    )(in_vmem(got), in_vmem(bias), gain, in_vmem(wqv), in_vmem(wk), in_vmem(proj))


def from_behind(value, axis, steps):
    count = lax.axis_size(axis)
    pairs = [(source, (source + steps) % count) for source in range(count)]
    return lax.ppermute(value, axis, pairs)


def exchange(value):
    order = tuple(range(lax.axis_size("band")))[::-1]
    return lax.all_to_all(
        value, "band", split_axis=0, concat_axis=0, axis_index_groups=[order], tiled=True
    )


def shards(
    pixels,
    keep_mask,
    band_counts,
    plan_dest,
    plan_slot,
    bias_table,
    gain_attn,
    qkv_weight,
    proj_weight,
    gain_mlp,
    hidden_weight,
    output_weight,
):
    gain_attn, gain_mlp = gain_attn[None], gain_mlp[None]
    pixels = jnp.transpose(pixels, (2, 0, 1))
    outgoing, top = spread(keep_mask, band_counts, plan_dest, plan_slot, pixels)
    halo = from_behind(top, "band", -1)
    gathered = exchange(outgoing)
    sent, kept, wqv, wk, proj, bias = own_path(
        keep_mask,
        band_counts,
        pixels,
        halo,
        bias_table.T,
        qkv_weight,
        proj_weight,
        gain_attn,
        gain_mlp,
        hidden_weight,
        output_weight.T,
    )
    upper = from_behind(sent, "band", 1)
    routed = route(gathered)
    incoming = exchange(routed)
    restored = jnp.concatenate([upper, kept], axis=1)
    restored = jnp.transpose(restored, (1, 2, 0))
    work_tiles = work_path(incoming, bias, gain_attn, wqv, wk, proj)
    work_tiles = jnp.transpose(work_tiles, (1, 2, 0))
    return (restored, work_tiles)


def solution(mesh):
    in_specs = (
        P(("img", "band"), None, None),
        P(("img", "band"), None),
        P(("img", "band")),
        P(("img", "band"), None),
        P(("img", "band"), None),
        P(),
        P(),
        P(),
        P(),
        P(),
        P(),
        P(),
    )
    out_specs = (P(("img", "band"), None, None), P(("img", "band"), None, None))
    return jax.shard_map(shards, mesh=mesh, in_specs=in_specs, out_specs=out_specs, check_vma=False)
```

```python
import jax
import jax.numpy as jnp
from jax import lax
from jax.experimental import pallas as pl
from jax.experimental.pallas import tpu as pltpu
from jax.sharding import PartitionSpec as P


CHAN = 180
HEADS = 6
HEAD_DIM = CHAN // HEADS
HEAD_PAD = 32
WIN = 8
TOKENS = WIN * WIN
TILE = 2
PAIR = TILE * TOKENS
SHIFT = 4
CAP = 8
TAIL = CHAN - 128
EPSILON = 1e-05

F32 = jnp.float32
BF16 = jnp.bfloat16


def dot(left, right, left_dim=1, right_dim=0):
    return lax.dot_general(
        left,
        right,
        (((left_dim,), (right_dim,)), ((), ())),
        preferred_element_type=F32,
    )


def layer_norm(values, gain):
    center = values - jnp.sum(values, axis=-1, keepdims=True) * (1.0 / CHAN)
    spread = jnp.sum(center * center, axis=-1, keepdims=True) * (1.0 / CHAN)
    return center * lax.rsqrt(spread + EPSILON) * gain


def iota(shape, dim):
    return lax.broadcasted_iota(jnp.int32, shape, dim)


def region_mask(row_flags, col_flags):
    shape = (TOKENS, PAIR)
    key, lane = iota(shape, 0), iota(shape, 1)
    first = lane < TOKENS
    row_differs = (((key >> 5) & 1) != ((lane >> 5) & 1)).astype(F32)
    col_differs = (((key >> 2) & 1) != ((lane >> 2) & 1)).astype(F32)
    row_on = jnp.where(first, row_flags[0], row_flags[1])
    col_on = jnp.where(first, col_flags[0], col_flags[1])
    return -100.0 * jnp.maximum(row_differs * row_on, col_differs * col_on)


def attend(x, masks, bias_ref, gain, wqv_ref, wk_ref):
    pairs = len(masks)
    normed = layer_norm(x, gain).astype(BF16)
    qv = dot(wqv_ref[...], normed, 1, 1)
    keys = dot(normed, wk_ref[...])
    key_low = (iota(keys.shape, 1) & 64) != 0
    keys = (keys - jnp.where(key_low, keys.astype(BF16).astype(F32), 0.0)).astype(BF16)
    half = HEADS * HEAD_PAD
    queries = qv[:half] * (HEAD_DIM ** (-0.5))
    high = queries.astype(BF16)
    low = (queries - high.astype(F32)).astype(BF16)
    values = qv[half:].astype(BF16)
    first_lane = iota((TOKENS, PAIR), 1) < TOKENS
    blank = jnp.zeros((PAIR, PAIR), BF16)
    scores = []
    for pair in range(pairs):
        lanes = slice(pair * PAIR, (pair + 1) * PAIR)
        for head in range(0, HEADS, 2):
            fours = []
            for one in (head, head + 1):
                rows = slice(one * HEAD_PAD, (one + 1) * HEAD_PAD)
                h, l = high[rows, lanes], low[rows, lanes]
                fours.append(jnp.concatenate([h, l, h, l], axis=0))
            both = jnp.concatenate(
                [
                    jnp.concatenate([fours[0], blank], axis=1),
                    jnp.concatenate([blank, fours[1]], axis=1),
                ],
                axis=0,
            )
            got = dot(keys[lanes, head * PAIR : (head + 2) * PAIR], both)
            for one in range(2):
                part = got[:, one * PAIR : (one + 1) * PAIR]
                scores.append(jnp.where(first_lane, part[:TOKENS], part[TOKENS:]))
    weights = []
    for pair in range(pairs):
        for head in range(HEADS):
            value = scores[pair * HEADS + head] + bias_ref[head] + masks[pair]
            value = jnp.exp(value - jnp.max(value, axis=0, keepdims=True))
            value = value * (1.0 / jnp.sum(value, axis=0, keepdims=True))
            weights.append(
                jnp.concatenate(
                    [jnp.where(first_lane, value, 0.0), jnp.where(first_lane, 0.0, value)], axis=0
                ).astype(BF16)
            )
    mixed = []
    for pair in range(pairs):
        lanes = slice(pair * PAIR, (pair + 1) * PAIR)
        parts = []
        for head in range(0, HEADS, 2):
            at = pair * HEADS + head
            both = jnp.concatenate([weights[at], weights[at + 1]], axis=1)
            rows = slice(head * HEAD_PAD, (head + 2) * HEAD_PAD)
            got = dot(values[rows, lanes], both)
            parts += [got[:HEAD_PAD, :PAIR], got[HEAD_PAD:, PAIR:]]
        mixed.append(jnp.concatenate(parts, axis=0).astype(BF16))
    return mixed


def feed(states, gain, hidden_ref, output_ref):
    normed = layer_norm(states, gain).astype(BF16)
    inner = jax.nn.gelu(dot(normed, hidden_ref[...]), approximate=True).astype(BF16)
    return states + dot(inner, output_ref[...], 1, 1)


def in_vmem(value):
    return pltpu.with_memory_space_constraint(value, pltpu.VMEM)


VMEM = pl.BlockSpec(memory_space=pltpu.VMEM)
SMEM = pl.BlockSpec(memory_space=pltpu.SMEM)


def pad_weights(qkv_ref, proj_ref, wqv_ref, wk_ref, padded_ref, turned_ref):
    half = HEADS * HEAD_PAD

    def source(column):
        inner = column & (HEAD_PAD - 1)
        return jnp.where(inner < HEAD_DIM, (column >> 5) * HEAD_DIM + inner, -1000)

    qkv = qkv_ref[...]
    column = iota((2 * half, 3 * CHAN), 0)
    wanted = jnp.where(column < half, source(column), 2 * CHAN + source(column - half))
    pick = (wanted == iota((2 * half, 3 * CHAN), 1)).astype(F32).astype(BF16)
    wqv_ref[...] = dot(pick, qkv, 1, 1).astype(BF16)
    shape = (3 * CHAN, HEADS * PAIR)
    column = iota(shape, 1)
    inner = column & (HEAD_PAD - 1)
    wanted = jnp.where(inner < HEAD_DIM, CHAN + (column >> 7) * HEAD_DIM + inner, -1)
    wk_ref[...] = dot(qkv, (wanted == iota(shape, 0)).astype(F32).astype(BF16)).astype(BF16)
    proj = proj_ref[...]
    pick = (source(iota((half, CHAN), 0)) == iota((half, CHAN), 1)).astype(F32).astype(BF16)
    padded_ref[...] = dot(pick, proj).astype(BF16)
    pick = (source(iota((CHAN, half), 1)) == iota((CHAN, half), 0)).astype(F32).astype(BF16)
    turned_ref[...] = dot(proj, pick, 0, 0).astype(BF16)


def spread_bias(table_ref, bias_ref, padded, looked):
    reach = 2 * WIN - 1
    padded[...] = jnp.zeros(padded.shape, F32)
    padded[0:HEADS, 0 : reach * reach] = table_ref[...]
    table = padded[...]
    for key in range(TOKENS):
        shift = 112 - (key // WIN) * reach - key % WIN
        moved = pltpu.roll(table, (256 - shift) % 256, 1)[:, :PAIR]
        looked[key * 8 : (key + 1) * 8, :] = moved
    rest = looked[...]
    query = iota((PAIR, PAIR), 1) & (TOKENS - 1)
    pick = (iota((PAIR, PAIR), 0) == (query >> 3) * reach + (query & 7)).astype(F32).astype(BF16)
    total = None
    for _ in range(3):
        part = rest.astype(BF16)
        rest = rest - part.astype(F32)
        got = dot(part, pick)
        total = got if total is None else total + got
    looked[...] = total
    for head in range(HEADS):
        bias_ref[head] = looked[pl.ds(head, TOKENS, stride=8), :]


def turned_rows(flat, row, stride):
    rows = pl.ds(row, 256, stride=stride)
    return jnp.concatenate([half[rows, :] for half in flat], axis=1).astype(BF16)


def hold_channels(block_ref, flat):
    channels, rows, _ = block_ref.shape
    for index, half in enumerate(flat):
        values = block_ref[:, :, index * 128 : (index + 1) * 128].astype(F32)
        half[0 : channels * rows, :] = values.reshape(channels * rows, 128)
        half[channels * rows :, :] = jnp.zeros((half.shape[0] - channels * rows, 128), F32)


def roll_pick(columns):
    wanted = (iota((columns, columns), 0) + SHIFT) & (columns - 1)
    return (wanted == iota((columns, columns), 1)).astype(F32).astype(BF16)


def own_kernel(
    pixels_ref,
    halo_ref,
    table_ref,
    qkv_ref,
    proj_ref,
    gain_attn_ref,
    gain_mlp_ref,
    hidden_ref,
    output_ref,
    sent_ref,
    kept_ref,
    wqv_ref,
    wk_ref,
    turned_ref,
    bias_ref,
    padded_proj,
    padded_table,
    looked,
    flat0,
    flat1,
    wide0,
    wide1,
    lower_rows,
    upper_rows,
    marks,
    finished,
):
    columns_all = pixels_ref.shape[2]
    pairs = 8
    steps = columns_all // (pairs * TILE * WIN)
    row_flag = jnp.where(lax.axis_index("band") == 0, 1.0, 0.0)
    pad_weights(qkv_ref, proj_ref, wqv_ref, wk_ref, padded_proj, turned_ref)
    spread_bias(table_ref, bias_ref, padded_table, looked)
    hold_channels(halo_ref, (flat0, flat1))
    hold_channels(pixels_ref, (wide0, wide1))
    pick = roll_pick(columns_all)
    for row in range(SHIFT):
        got = dot(pick, turned_rows((flat0, flat1), row, SHIFT), 1, 1)
        upper_rows[row] = got[:, :CHAN]
        if row == 0:
            marks[...] = got[:, 128:]
        got = dot(pick, turned_rows((wide0, wide1), row, WIN), 1, 1)
        lower_rows[row] = got[:, :CHAN]

    def some_pairs(step, carry):
        tokens, masks = [], []
        for pair in range(pairs):
            start = pl.multiple_of((step * pairs + pair) * TILE * WIN, TILE * WIN)
            columns = pl.ds(start, TILE * WIN)
            upper = upper_rows[:, columns, :]
            lower = lower_rows[:, columns, :]
            for w in range(TILE):
                for part in (upper, lower):
                    tokens.append(
                        part[:, w * WIN : (w + 1) * WIN].reshape(SHIFT * WIN, CHAN)
                    )
            at_end = jnp.where((step == steps - 1) & (pair == pairs - 1), 1.0, 0.0)
            masks.append(region_mask((row_flag, row_flag), (0.0, at_end)))
        x = jnp.concatenate(tokens, axis=0)
        mixed = attend(x, masks, bias_ref, gain_attn_ref[...], wqv_ref, wk_ref)
        projected = [dot(part, padded_proj[...], 0, 0) for part in mixed]
        attended = x + jnp.concatenate(projected, axis=0)
        attended = attended.astype(BF16).astype(F32)
        done = feed(attended, gain_mlp_ref[...], hidden_ref, output_ref)
        for pair in range(pairs):
            start = pl.multiple_of((step * pairs + pair) * TILE * WIN, TILE * WIN)
            kept = []
            for w in range(TILE):
                at = pair * TILE + w
                rows = slice(at * TOKENS, (at + 1) * TOKENS)
                on = marks[pl.ds(start + w * WIN, WIN), :][0:1, TAIL : TAIL + 1] > 0.5
                kept.append(jnp.where(on, done[rows], x[rows]).reshape(WIN, WIN, CHAN))
            kept = jnp.concatenate(kept, axis=1).astype(BF16)
            finished[:, pl.ds(start, TILE * WIN), :] = kept
        return carry

    lax.fori_loop(0, steps, some_pairs, 0)

    same = (iota((CHAN, CHAN), 0) == iota((CHAN, CHAN), 1)).astype(F32).astype(BF16)
    for first, out_ref in ((0, sent_ref), (SHIFT, kept_ref)):
        for row in range(SHIFT):
            got = pltpu.roll(dot(same, finished[first + row], 1, 1), SHIFT, 1)
            rows = pl.ds(row, CHAN, stride=SHIFT)
            flat0[rows, :] = got[:, :128]
            flat1[rows, :] = got[:, 128:]
        for index, flat in enumerate((flat0, flat1)):
            values = flat[0 : CHAN * SHIFT, :].reshape(CHAN, SHIFT, 128)
            out_ref[:, :, index * 128 : (index + 1) * 128] = values.astype(BF16)


def own_path(pixels, halo, table, qkv, proj, gain_attn, gain_mlp, hidden, output):
    columns = pixels.shape[2]
    half = HEADS * HEAD_PAD
    flat = pltpu.VMEM((256 * SHIFT, 128), F32)
    wide = pltpu.VMEM((256 * WIN, 128), F32)
    rows = pltpu.VMEM((SHIFT, columns, CHAN), F32)
    part = jax.ShapeDtypeStruct((CHAN, SHIFT, columns), BF16)
    return pl.pallas_call(
        own_kernel,
        in_specs=[VMEM] * 9,
        out_specs=[VMEM] * 6,
        out_shape=[
            part,
            part,
            pltpu.VMEM((2 * half, CHAN), BF16),
            pltpu.VMEM((CHAN, HEADS * PAIR), BF16),
            pltpu.VMEM((CHAN, half), BF16),
            pltpu.VMEM((HEADS, TOKENS, PAIR), F32),
        ],
        scratch_shapes=[
            pltpu.VMEM((half, CHAN), BF16),
            pltpu.VMEM((8, 256), F32),
            pltpu.VMEM((8 * TOKENS, PAIR), F32),
            flat,
            flat,
            wide,
            wide,
            rows,
            rows,
            pltpu.VMEM((columns, 128), F32),
            pltpu.VMEM((WIN, columns, CHAN), BF16),
        ],
        cost_estimate=pl.CostEstimate(
            flops=20_000_000_000, bytes_accessed=3_000_000, transcendentals=2_000_000
        ),
        name="own_path",
    )(pixels, in_vmem(halo), table, qkv, proj, gain_attn, gain_mlp, hidden, output)


def spread_kernel(
    keep_ref,
    count_ref,
    dest_ref,
    slot_ref,
    pixels_ref,
    out_ref,
    edge_ref,
    flat0,
    flat1,
):
    channels, rows, columns = pixels_ref.shape
    windows = columns // WIN
    half = windows // 2
    bands = lax.axis_size("band")
    last_band = jnp.where(lax.axis_index("band") == bands - 1, 1.0, 0.0)
    row, lane = iota((half, 128), 0), iota((half, 128), 1) - 2 * TAIL
    codes = jnp.where((lane == 4) | (lane == 6), last_band, 0.0)
    codes = jnp.where((lane == 7) & (row == half - 1), 1.0, codes)
    window_of = ((iota((SHIFT, columns), 1) - SHIFT) & (columns - 1)) >> 3
    running = jnp.zeros((SHIFT, columns), F32)
    position = jnp.int32(-1)
    for w in range(windows):
        keep = keep_ref[0, w]
        position = position + keep
        tile = jnp.maximum(position, 0) >> 1
        slot = slot_ref[0, tile]
        active = (keep == 1) & (position < count_ref[0])
        running = jnp.where(window_of == w, jnp.where(active, 1.0, 0.0), running)
        placed = active & (slot < CAP)
        dest = jnp.where(placed, bands - 1 - dest_ref[0, tile], bands).astype(F32)
        place = jnp.where(placed, slot * TILE + (position & 1), 0).astype(F32)
        first = 2 * (w // half)
        here = row == w % half
        codes = jnp.where(here & (lane == first), dest, codes)
        codes = jnp.where(here & (lane == first + 1), place, codes)

    edge_ref[0:channels] = pixels_ref[:, SHIFT:, :]
    edge_ref[channels] = running.astype(BF16)
    extra = edge_ref.shape[0] - channels - 1
    edge_ref[channels + 1 :] = jnp.zeros((extra, SHIFT, columns), BF16)
    hold_channels(pixels_ref, (flat0, flat1))
    out_row = iota((columns, columns), 0)
    wanted = ((out_row & (windows - 1)) * WIN + (out_row >> 5) + SHIFT) & (columns - 1)
    group = (wanted == iota((columns, columns), 1)).astype(F32).astype(BF16)
    for r in range(rows):
        got = dot(group, turned_rows((flat0, flat1), r, rows), 1, 1)
        for cu in range(WIN):
            token = (r + SHIFT) % rows * WIN + cu
            low = got[cu * windows : cu * windows + half]
            high = got[cu * windows + half : (cu + 1) * windows]
            packed = low[:, 128:] + pltpu.roll(high[:, 128:], TAIL, 1) + codes
            out_ref[token, :, 0:128] = low[:, :128].astype(BF16)
            out_ref[token, :, 128:256] = high[:, :128].astype(BF16)
            out_ref[token, :, 256:384] = packed.astype(BF16)


def spread(keep, count, dest, slot, pixels):
    channels, rows, columns = pixels.shape
    half = columns // WIN // 2
    flat = pltpu.VMEM((256 * rows, 128), F32)
    return pl.pallas_call(
        spread_kernel,
        in_specs=[SMEM] * 4 + [VMEM],
        out_specs=[VMEM] * 2,
        out_shape=[
            jax.ShapeDtypeStruct((TOKENS, half, 384), BF16),
            jax.ShapeDtypeStruct((channels + 4, SHIFT, columns), BF16),
        ],
        scratch_shapes=[flat, flat],
        cost_estimate=pl.CostEstimate(
            flops=500_000_000, bytes_accessed=2_000_000, transcendentals=0
        ),
        name="spread",
    )(keep, count, dest, slot, pixels)


def route_kernel(got_ref, out_ref):
    bands, half, _ = got_ref.shape
    slots = out_ref.shape[0] * out_ref.shape[1]
    sources = bands * half
    got = got_ref[...].reshape(sources, 384)
    tails = got[:, 256:384]
    row = iota((8, 128), 0)
    lane = iota((8, 128), 1) - 2 * TAIL - 2 * row
    pick = jnp.where(row < 2, jnp.where(lane == 0, 16.0, jnp.where(lane == 1, 1.0, 0.0)), 0.0)
    codes = dot(pick.astype(BF16), tails, 1, 1)
    behind = bands - 1 - lax.axis_index("band") >= TOKENS // 2
    codes = jnp.where(behind, pltpu.roll(codes, sources - half, 1), codes)
    low, high = codes[0:1].astype(jnp.int32), codes[1:2].astype(jnp.int32)
    chunk = 256
    lane_out = iota((chunk, 128), 1)
    is_kind = (lane_out == 2 * TAIL + 4) | (lane_out == 2 * TAIL + 5)
    first = jnp.concatenate([got[:, 0:128], tails], axis=1)
    second = jnp.concatenate([got[:, 128:256], tails], axis=1)
    for start in range(0, slots, chunk):
        target = (iota((chunk, sources), 0) + start) * TILE
        heads, total = [], None
        for place in range(TILE):
            pick_low = jnp.where(target + place == low, 1.0, 0.0).astype(BF16)
            pick_high = jnp.where(target + place == high, 1.0, 0.0).astype(BF16)
            from_low = dot(pick_low, first)
            from_high = dot(pick_high, second)
            heads.append(from_low[:, 0:128] + from_high[:, 0:128])
            low_tail, high_tail = from_low[:, 128:256], from_high[:, 128:256]
            tail = low_tail + pltpu.roll(high_tail, 128 - TAIL, 1)
            kind = low_tail + pltpu.roll(high_tail, 126, 1)
            tail = jnp.where(lane_out < TAIL, tail, 0.0)
            kind = jnp.where(is_kind, kind, 0.0)
            if place:
                tail = pltpu.roll(tail, TAIL, 1)
                kind = pltpu.roll(kind, 2, 1)
            total = tail + kind if total is None else total + tail + kind
        out = out_ref.at[start // CAP : (start + chunk) // CAP]
        blocks = chunk // CAP
        out[:, :, 0:128] = heads[0].reshape(blocks, CAP, 128).astype(BF16)
        out[:, :, 128:256] = heads[1].reshape(blocks, CAP, 128).astype(BF16)
        out[:, :, 256:384] = total.reshape(blocks, CAP, 128).astype(BF16)


def route(got):
    bands = got.shape[0]
    return pl.pallas_call(
        route_kernel,
        in_specs=[VMEM],
        out_specs=VMEM,
        out_shape=jax.ShapeDtypeStruct((bands, CAP, 384), BF16),
        cost_estimate=pl.CostEstimate(
            flops=1_200_000_000, bytes_accessed=1_200_000, transcendentals=0
        ),
        name="route",
    )(in_vmem(got))


def work_kernel(got_ref, bias_ref, gain_ref, wqv_ref, wk_ref, proj_ref, out_ref, held, done):
    for part in range(held.shape[0]):
        values = got_ref[:, :, part * 128 : (part + 1) * 128].astype(F32)
        held[part] = values.reshape(TOKENS * CAP, 128)
    pairs = 8

    def some_slots(step, carry):
        tokens, masks = [], []
        for index in range(pairs):
            slot = step * pairs + index
            rows = pl.ds(slot, TOKENS, stride=CAP)
            tail = held[TILE, rows, :]
            for place in range(TILE):
                head = held[place, rows, :]
                moved = pltpu.roll(tail, 128 - TAIL, 1) if place else tail
                tokens.append(jnp.concatenate([head, moved], axis=1)[:, :CHAN])
            lane = iota((1, 128), 1) - 2 * TAIL - 4
            flags = [
                jnp.sum(jnp.where(lane == i, tail[0:1], 0.0), axis=1, keepdims=True)
                for i in range(4)
            ]
            masks.append(region_mask(flags[0::2], flags[1::2]))
        x = jnp.concatenate(tokens, axis=0)
        mixed = attend(x, masks, bias_ref, gain_ref[...], wqv_ref, wk_ref)
        for index in range(pairs):
            rows = pl.ds(step * pairs + index, CHAN, stride=CAP)
            own = x[index * PAIR : (index + 1) * PAIR]
            done[rows, :] = own.T + dot(proj_ref[...], mixed[index])
        return carry

    lax.fori_loop(0, CAP // pairs, some_slots, 0)
    out_ref[...] = done[...].reshape(CHAN, CAP, PAIR).astype(BF16)


def work_path(got, bias, gain, wqv, wk, proj):
    return pl.pallas_call(
        work_kernel,
        in_specs=[VMEM] * 6,
        out_specs=VMEM,
        out_shape=jax.ShapeDtypeStruct((CHAN, CAP, PAIR), BF16),
        scratch_shapes=[
            pltpu.VMEM((TILE + 1, TOKENS * CAP, 128), F32),
            pltpu.VMEM((CHAN * CAP, PAIR), F32),
        ],
        cost_estimate=pl.CostEstimate(
            flops=8_000_000_000, bytes_accessed=2_000_000, transcendentals=1_000_000
        ),
        name="work_path",
    )(in_vmem(got), in_vmem(bias), gain, in_vmem(wqv), in_vmem(wk), in_vmem(proj))


def from_behind(value, axis, steps):
    count = lax.axis_size(axis)
    pairs = [(source, (source + steps) % count) for source in range(count)]
    return lax.ppermute(value, axis, pairs)


def exchange(value):
    order = tuple(range(lax.axis_size("band")))[::-1]
    return lax.all_to_all(
        value, "band", split_axis=0, concat_axis=0, axis_index_groups=[order], tiled=True
    )


def shards(
    pixels,
    keep_mask,
    band_counts,
    plan_dest,
    plan_slot,
    bias_table,
    gain_attn,
    qkv_weight,
    proj_weight,
    gain_mlp,
    hidden_weight,
    output_weight,
):
    gain_attn, gain_mlp = gain_attn[None], gain_mlp[None]
    pixels = jnp.transpose(pixels, (2, 0, 1))
    outgoing, edge = spread(keep_mask, band_counts, plan_dest, plan_slot, pixels)
    halo = from_behind(edge, "band", 1)
    gathered = exchange(outgoing)
    sent, kept, wqv, wk, proj, bias = own_path(
        pixels,
        halo,
        bias_table.T,
        qkv_weight,
        proj_weight,
        gain_attn,
        gain_mlp,
        hidden_weight,
        output_weight.T,
    )
    lower = from_behind(sent, "band", -1)
    routed = route(gathered)
    incoming = exchange(routed)
    restored = jnp.concatenate([kept, lower], axis=1)
    restored = jnp.transpose(restored, (1, 2, 0))
    work_tiles = work_path(incoming, bias, gain_attn, wqv, wk, proj)
    work_tiles = jnp.transpose(work_tiles, (1, 2, 0))
    return (restored, work_tiles)


def solution(mesh):
    in_specs = (
        P(("img", "band"), None, None),
        P(("img", "band"), None),
        P(("img", "band")),
        P(("img", "band"), None),
        P(("img", "band"), None),
        P(),
        P(),
        P(),
        P(),
        P(),
        P(),
        P(),
    )
    out_specs = (P(("img", "band"), None, None), P(("img", "band"), None, None))
    return jax.shard_map(shards, mesh=mesh, in_specs=in_specs, out_specs=out_specs, check_vma=False)
```

```python
import jax
import jax.numpy as jnp
from jax import lax
from jax.experimental import pallas as pl
from jax.experimental.pallas import tpu as pltpu
from jax.sharding import PartitionSpec as P


CHAN = 180
HEADS = 6
HEAD_DIM = CHAN // HEADS
HEAD_PAD = 32
WIN = 8
TOKENS = WIN * WIN
TILE = 2
PAIR = TILE * TOKENS
SHIFT = 4
CAP = 8
TAIL = CHAN - 128
LEAD = 41
EPSILON = 1e-05

F32 = jnp.float32
BF16 = jnp.bfloat16


def dot(left, right, left_dim=1, right_dim=0):
    return lax.dot_general(
        left,
        right,
        (((left_dim,), (right_dim,)), ((), ())),
        preferred_element_type=F32,
    )


def layer_norm(values, gain):
    center = values - jnp.sum(values, axis=-1, keepdims=True) * (1.0 / CHAN)
    spread = jnp.sum(center * center, axis=-1, keepdims=True) * (1.0 / CHAN)
    return center * lax.rsqrt(spread + EPSILON) * gain


def iota(shape, dim):
    return lax.broadcasted_iota(jnp.int32, shape, dim)


def region_mask(row_flags, col_flags):
    shape = (TOKENS, PAIR)
    key, lane = iota(shape, 0), iota(shape, 1)
    first = lane < TOKENS
    row_differs = (((key >> 5) & 1) != ((lane >> 5) & 1)).astype(F32)
    col_differs = (((key >> 2) & 1) != ((lane >> 2) & 1)).astype(F32)
    row_on = jnp.where(first, row_flags[0], row_flags[1])
    col_on = jnp.where(first, col_flags[0], col_flags[1])
    return -100.0 * jnp.maximum(row_differs * row_on, col_differs * col_on)


def attend(x, masks, bias_ref, gain, wqv_ref, wk_ref):
    pairs = len(masks)
    normed = layer_norm(x, gain).astype(BF16)
    qv = dot(wqv_ref[...], normed, 1, 1)
    keys = dot(normed, wk_ref[...])
    key_low = (iota(keys.shape, 1) & 64) != 0
    keys = (keys - jnp.where(key_low, keys.astype(BF16).astype(F32), 0.0)).astype(BF16)
    half = HEADS * HEAD_PAD
    queries = qv[:half] * (HEAD_DIM ** (-0.5))
    high = queries.astype(BF16)
    low = (queries - high.astype(F32)).astype(BF16)
    values = qv[half:].astype(BF16)
    first_lane = iota((TOKENS, PAIR), 1) < TOKENS
    blank = jnp.zeros((PAIR, PAIR), BF16)
    scores = []
    for pair in range(pairs):
        lanes = slice(pair * PAIR, (pair + 1) * PAIR)
        for head in range(0, HEADS, 2):
            fours = []
            for one in (head, head + 1):
                rows = slice(one * HEAD_PAD, (one + 1) * HEAD_PAD)
                h, l = high[rows, lanes], low[rows, lanes]
                fours.append(jnp.concatenate([h, l, h, l], axis=0))
            both = jnp.concatenate(
                [
                    jnp.concatenate([fours[0], blank], axis=1),
                    jnp.concatenate([blank, fours[1]], axis=1),
                ],
                axis=0,
            )
            got = dot(keys[lanes, head * PAIR : (head + 2) * PAIR], both)
            for one in range(2):
                part = got[:, one * PAIR : (one + 1) * PAIR]
                scores.append(jnp.where(first_lane, part[:TOKENS], part[TOKENS:]))
    weights = []
    for pair in range(pairs):
        for head in range(HEADS):
            value = scores[pair * HEADS + head] + bias_ref[head] + masks[pair]
            value = jnp.exp(value - jnp.max(value, axis=0, keepdims=True))
            value = value * (1.0 / jnp.sum(value, axis=0, keepdims=True))
            weights.append(
                jnp.concatenate(
                    [jnp.where(first_lane, value, 0.0), jnp.where(first_lane, 0.0, value)], axis=0
                ).astype(BF16)
            )
    mixed = []
    for pair in range(pairs):
        lanes = slice(pair * PAIR, (pair + 1) * PAIR)
        parts = []
        for head in range(0, HEADS, 2):
            at = pair * HEADS + head
            both = jnp.concatenate([weights[at], weights[at + 1]], axis=1)
            rows = slice(head * HEAD_PAD, (head + 2) * HEAD_PAD)
            got = dot(values[rows, lanes], both)
            parts += [got[:HEAD_PAD, :PAIR], got[HEAD_PAD:, PAIR:]]
        mixed.append(jnp.concatenate(parts, axis=0).astype(BF16))
    return mixed


def feed(states, gain, hidden_ref, output_ref):
    normed = layer_norm(states, gain).astype(BF16)
    inner = jax.nn.gelu(dot(normed, hidden_ref[...]), approximate=True).astype(BF16)
    return states + dot(inner, output_ref[...], 1, 1)


def in_vmem(value):
    return pltpu.with_memory_space_constraint(value, pltpu.VMEM)


VMEM = pl.BlockSpec(memory_space=pltpu.VMEM)
SMEM = pl.BlockSpec(memory_space=pltpu.SMEM)


def pad_weights(qkv_ref, proj_ref, wqv_ref, wk_ref, padded_ref, turned_ref):
    half = HEADS * HEAD_PAD

    def source(column):
        inner = column & (HEAD_PAD - 1)
        return jnp.where(inner < HEAD_DIM, (column >> 5) * HEAD_DIM + inner, -1000)

    qkv = qkv_ref[...]
    column = iota((2 * half, 3 * CHAN), 0)
    wanted = jnp.where(column < half, source(column), 2 * CHAN + source(column - half))
    pick = (wanted == iota((2 * half, 3 * CHAN), 1)).astype(F32).astype(BF16)
    wqv_ref[...] = dot(pick, qkv, 1, 1).astype(BF16)
    shape = (3 * CHAN, HEADS * PAIR)
    column = iota(shape, 1)
    inner = column & (HEAD_PAD - 1)
    wanted = jnp.where(inner < HEAD_DIM, CHAN + (column >> 7) * HEAD_DIM + inner, -1)
    wk_ref[...] = dot(qkv, (wanted == iota(shape, 0)).astype(F32).astype(BF16)).astype(BF16)
    proj = proj_ref[...]
    pick = (source(iota((half, CHAN), 0)) == iota((half, CHAN), 1)).astype(F32).astype(BF16)
    padded_ref[...] = dot(pick, proj).astype(BF16)
    pick = (source(iota((CHAN, half), 1)) == iota((CHAN, half), 0)).astype(F32).astype(BF16)
    turned_ref[...] = dot(proj, pick, 0, 0).astype(BF16)


def spread_bias(table_ref, bias_ref, padded, looked):
    reach = 2 * WIN - 1
    padded[...] = jnp.zeros(padded.shape, F32)
    padded[0:HEADS, 0 : reach * reach] = table_ref[...]
    table = padded[...]
    for key in range(TOKENS):
        shift = 112 - (key // WIN) * reach - key % WIN
        moved = pltpu.roll(table, (256 - shift) % 256, 1)[:, :PAIR]
        looked[key * 8 : (key + 1) * 8, :] = moved
    rest = looked[...]
    query = iota((PAIR, PAIR), 1) & (TOKENS - 1)
    pick = (iota((PAIR, PAIR), 0) == (query >> 3) * reach + (query & 7)).astype(F32).astype(BF16)
    total = None
    for _ in range(3):
        part = rest.astype(BF16)
        rest = rest - part.astype(F32)
        got = dot(part, pick)
        total = got if total is None else total + got
    looked[...] = total
    for head in range(HEADS):
        bias_ref[head] = looked[pl.ds(head, TOKENS, stride=8), :]


def turned_rows(flat, row, stride):
    rows = pl.ds(row, 256, stride=stride)
    return jnp.concatenate([half[rows, :] for half in flat], axis=1).astype(BF16)


def hold_channels(block_ref, flat):
    channels, rows, _ = block_ref.shape
    for index, half in enumerate(flat):
        values = block_ref[:, :, index * 128 : (index + 1) * 128].astype(F32)
        half[0 : channels * rows, :] = values.reshape(channels * rows, 128)
        half[channels * rows :, :] = jnp.zeros((half.shape[0] - channels * rows, 128), F32)


def roll_pick(columns):
    wanted = (iota((columns, columns), 0) + SHIFT) & (columns - 1)
    return (wanted == iota((columns, columns), 1)).astype(F32).astype(BF16)


def own_kernel(
    pixels_ref,
    halo_ref,
    table_ref,
    qkv_ref,
    proj_ref,
    gain_attn_ref,
    gain_mlp_ref,
    hidden_ref,
    output_ref,
    sent_ref,
    kept_ref,
    wqv_ref,
    wk_ref,
    turned_ref,
    bias_ref,
    padded_proj,
    padded_table,
    looked,
    flat0,
    flat1,
    wide0,
    wide1,
    lower_rows,
    upper_rows,
    marks,
    finished,
):
    columns_all = pixels_ref.shape[2]
    pairs = 8
    steps = columns_all // (pairs * TILE * WIN)
    row_flag = jnp.where(lax.axis_index("band") == 0, 1.0, 0.0)
    pad_weights(qkv_ref, proj_ref, wqv_ref, wk_ref, padded_proj, turned_ref)
    spread_bias(table_ref, bias_ref, padded_table, looked)
    hold_channels(halo_ref, (flat0, flat1))
    hold_channels(pixels_ref, (wide0, wide1))
    pick = roll_pick(columns_all)
    for row in range(SHIFT):
        got = dot(pick, turned_rows((flat0, flat1), row, SHIFT), 1, 1)
        upper_rows[row] = got[:, :CHAN]
        if row == 0:
            marks[...] = got[:, 128:]
        got = dot(pick, turned_rows((wide0, wide1), row, WIN), 1, 1)
        lower_rows[row] = got[:, :CHAN]

    def some_pairs(step, carry):
        tokens, masks = [], []
        for pair in range(pairs):
            start = pl.multiple_of((step * pairs + pair) * TILE * WIN, TILE * WIN)
            columns = pl.ds(start, TILE * WIN)
            upper = upper_rows[:, columns, :]
            lower = lower_rows[:, columns, :]
            for w in range(TILE):
                for part in (upper, lower):
                    tokens.append(
                        part[:, w * WIN : (w + 1) * WIN].reshape(SHIFT * WIN, CHAN)
                    )
            at_end = jnp.where((step == steps - 1) & (pair == pairs - 1), 1.0, 0.0)
            masks.append(region_mask((row_flag, row_flag), (0.0, at_end)))
        x = jnp.concatenate(tokens, axis=0)
        mixed = attend(x, masks, bias_ref, gain_attn_ref[...], wqv_ref, wk_ref)
        projected = [dot(part, padded_proj[...], 0, 0) for part in mixed]
        attended = x + jnp.concatenate(projected, axis=0)
        attended = attended.astype(BF16).astype(F32)
        done = feed(attended, gain_mlp_ref[...], hidden_ref, output_ref)
        for pair in range(pairs):
            start = pl.multiple_of((step * pairs + pair) * TILE * WIN, TILE * WIN)
            kept = []
            for w in range(TILE):
                at = pair * TILE + w
                rows = slice(at * TOKENS, (at + 1) * TOKENS)
                on = marks[pl.ds(start + w * WIN, WIN), :][0:1, TAIL : TAIL + 1] > 0.5
                kept.append(jnp.where(on, done[rows], x[rows]).reshape(WIN, WIN, CHAN))
            kept = jnp.concatenate(kept, axis=1).astype(BF16)
            finished[:, pl.ds(start, TILE * WIN), :] = kept
        return carry

    lax.fori_loop(0, steps, some_pairs, 0)

    same = (iota((CHAN, CHAN), 0) == iota((CHAN, CHAN), 1)).astype(F32).astype(BF16)
    for first, out_ref in ((0, sent_ref), (SHIFT, kept_ref)):
        for row in range(SHIFT):
            got = pltpu.roll(dot(same, finished[first + row], 1, 1), SHIFT, 1)
            rows = pl.ds(row, CHAN, stride=SHIFT)
            flat0[rows, :] = got[:, :128]
            flat1[rows, :] = got[:, 128:]
        for index, flat in enumerate((flat0, flat1)):
            values = flat[0 : CHAN * SHIFT, :].reshape(CHAN, SHIFT, 128)
            out_ref[:, :, index * 128 : (index + 1) * 128] = values.astype(BF16)


def own_path(pixels, halo, table, qkv, proj, gain_attn, gain_mlp, hidden, output):
    columns = pixels.shape[2]
    half = HEADS * HEAD_PAD
    flat = pltpu.VMEM((256 * SHIFT, 128), F32)
    wide = pltpu.VMEM((256 * WIN, 128), F32)
    rows = pltpu.VMEM((SHIFT, columns, CHAN), F32)
    part = jax.ShapeDtypeStruct((CHAN, SHIFT, columns), BF16)
    return pl.pallas_call(
        own_kernel,
        in_specs=[VMEM] * 9,
        out_specs=[VMEM] * 6,
        out_shape=[
            part,
            part,
            pltpu.VMEM((2 * half, CHAN), BF16),
            pltpu.VMEM((CHAN, HEADS * PAIR), BF16),
            pltpu.VMEM((CHAN, half), BF16),
            pltpu.VMEM((HEADS, TOKENS, PAIR), F32),
        ],
        scratch_shapes=[
            pltpu.VMEM((half, CHAN), BF16),
            pltpu.VMEM((8, 256), F32),
            pltpu.VMEM((8 * TOKENS, PAIR), F32),
            flat,
            flat,
            wide,
            wide,
            rows,
            rows,
            pltpu.VMEM((columns, 128), F32),
            pltpu.VMEM((WIN, columns, CHAN), BF16),
        ],
        cost_estimate=pl.CostEstimate(
            flops=20_000_000_000, bytes_accessed=3_000_000, transcendentals=2_000_000
        ),
        name="own_path",
    )(pixels, in_vmem(halo), table, qkv, proj, gain_attn, gain_mlp, hidden, output)


def spread_kernel(
    keep_ref,
    count_ref,
    dest_ref,
    slot_ref,
    pixels_ref,
    out_ref,
    edge_ref,
    flat0,
    flat1,
):
    channels, rows, columns = pixels_ref.shape
    windows = columns // WIN
    half = windows // 2
    bands = lax.axis_size("band")
    last_band = jnp.where(lax.axis_index("band") == bands - 1, 1.0, 0.0)
    row, lane = iota((half, 128), 0), iota((half, 128), 1) - 2 * TAIL
    codes = jnp.where((lane == 4) | (lane == 6), last_band, 0.0)
    codes = jnp.where((lane == 7) & (row == half - 1), 1.0, codes)
    window_of = ((iota((SHIFT, columns), 1) - SHIFT) & (columns - 1)) >> 3
    running = jnp.zeros((SHIFT, columns), F32)
    position = jnp.int32(-1)
    for w in range(windows):
        keep = keep_ref[0, w]
        position = position + keep
        tile = jnp.maximum(position, 0) >> 1
        slot = slot_ref[0, tile]
        active = (keep == 1) & (position < count_ref[0])
        running = jnp.where(window_of == w, jnp.where(active, 1.0, 0.0), running)
        placed = active & (slot < CAP)
        dest = jnp.where(placed, (LEAD - dest_ref[0, tile]) & (bands - 1), bands).astype(F32)
        place = jnp.where(placed, slot * TILE + (position & 1), 0).astype(F32)
        first = 2 * (w // half)
        here = row == w % half
        codes = jnp.where(here & (lane == first), dest, codes)
        codes = jnp.where(here & (lane == first + 1), place, codes)

    edge_ref[0:channels] = pixels_ref[:, SHIFT:, :]
    edge_ref[channels] = running.astype(BF16)
    extra = edge_ref.shape[0] - channels - 1
    edge_ref[channels + 1 :] = jnp.zeros((extra, SHIFT, columns), BF16)
    hold_channels(pixels_ref, (flat0, flat1))
    out_row = iota((columns, columns), 0)
    wanted = ((out_row & (windows - 1)) * WIN + (out_row >> 5) + SHIFT) & (columns - 1)
    group = (wanted == iota((columns, columns), 1)).astype(F32).astype(BF16)
    for r in range(rows):
        got = dot(group, turned_rows((flat0, flat1), r, rows), 1, 1)
        for cu in range(WIN):
            token = (r + SHIFT) % rows * WIN + cu
            low = got[cu * windows : cu * windows + half]
            high = got[cu * windows + half : (cu + 1) * windows]
            packed = low[:, 128:] + pltpu.roll(high[:, 128:], TAIL, 1) + codes
            out_ref[token, :, 0:128] = low[:, :128].astype(BF16)
            out_ref[token, :, 128:256] = high[:, :128].astype(BF16)
            out_ref[token, :, 256:384] = packed.astype(BF16)


def spread(keep, count, dest, slot, pixels):
    channels, rows, columns = pixels.shape
    half = columns // WIN // 2
    flat = pltpu.VMEM((256 * rows, 128), F32)
    return pl.pallas_call(
        spread_kernel,
        in_specs=[SMEM] * 4 + [VMEM],
        out_specs=[VMEM] * 2,
        out_shape=[
            jax.ShapeDtypeStruct((TOKENS, half, 384), BF16),
            pltpu.VMEM((channels + 4, SHIFT, columns), BF16),
        ],
        scratch_shapes=[flat, flat],
        cost_estimate=pl.CostEstimate(
            flops=500_000_000, bytes_accessed=2_000_000, transcendentals=0
        ),
        name="spread",
    )(keep, count, dest, slot, pixels)


def route_kernel(got_ref, out_ref):
    bands, half, _ = got_ref.shape
    slots = out_ref.shape[0] * out_ref.shape[1]
    sources = bands * half
    got = got_ref[...].reshape(sources, 384)
    tails = got[:, 256:384]
    row = iota((8, 128), 0)
    lane = iota((8, 128), 1) - 2 * TAIL - 2 * row
    pick = jnp.where(row < 2, jnp.where(lane == 0, 16.0, jnp.where(lane == 1, 1.0, 0.0)), 0.0)
    codes = dot(pick.astype(BF16), tails, 1, 1)
    behind = (LEAD - lax.axis_index("band")) & (bands - 1) >= TOKENS // 2
    codes = jnp.where(behind, pltpu.roll(codes, sources - half, 1), codes)
    low, high = codes[0:1].astype(jnp.int32), codes[1:2].astype(jnp.int32)
    chunk = 256
    lane_out = iota((chunk, 128), 1)
    is_kind = (lane_out == 2 * TAIL + 4) | (lane_out == 2 * TAIL + 5)
    first = jnp.concatenate([got[:, 0:128], tails], axis=1)
    second = jnp.concatenate([got[:, 128:256], tails], axis=1)
    for start in range(0, slots, chunk):
        target = (iota((chunk, sources), 0) + start) * TILE
        heads, total = [], None
        for place in range(TILE):
            pick_low = jnp.where(target + place == low, 1.0, 0.0).astype(BF16)
            pick_high = jnp.where(target + place == high, 1.0, 0.0).astype(BF16)
            from_low = dot(pick_low, first)
            from_high = dot(pick_high, second)
            heads.append(from_low[:, 0:128] + from_high[:, 0:128])
            low_tail, high_tail = from_low[:, 128:256], from_high[:, 128:256]
            tail = low_tail + pltpu.roll(high_tail, 128 - TAIL, 1)
            kind = low_tail + pltpu.roll(high_tail, 126, 1)
            tail = jnp.where(lane_out < TAIL, tail, 0.0)
            kind = jnp.where(is_kind, kind, 0.0)
            if place:
                tail = pltpu.roll(tail, TAIL, 1)
                kind = pltpu.roll(kind, 2, 1)
            total = tail + kind if total is None else total + tail + kind
        out = out_ref.at[start // CAP : (start + chunk) // CAP]
        blocks = chunk // CAP
        out[:, :, 0:128] = heads[0].reshape(blocks, CAP, 128).astype(BF16)
        out[:, :, 128:256] = heads[1].reshape(blocks, CAP, 128).astype(BF16)
        out[:, :, 256:384] = total.reshape(blocks, CAP, 128).astype(BF16)


def route(got):
    bands = got.shape[0]
    return pl.pallas_call(
        route_kernel,
        in_specs=[VMEM],
        out_specs=VMEM,
        out_shape=jax.ShapeDtypeStruct((bands, CAP, 384), BF16),
        cost_estimate=pl.CostEstimate(
            flops=1_200_000_000, bytes_accessed=1_200_000, transcendentals=0
        ),
        name="route",
    )(in_vmem(got))


def work_kernel(got_ref, bias_ref, gain_ref, wqv_ref, wk_ref, proj_ref, out_ref, held, done):
    for part in range(held.shape[0]):
        values = got_ref[:, :, part * 128 : (part + 1) * 128].astype(F32)
        held[part] = values.reshape(TOKENS * CAP, 128)
    pairs = 8

    def some_slots(step, carry):
        tokens, masks = [], []
        for index in range(pairs):
            slot = step * pairs + index
            rows = pl.ds(slot, TOKENS, stride=CAP)
            tail = held[TILE, rows, :]
            for place in range(TILE):
                head = held[place, rows, :]
                moved = pltpu.roll(tail, 128 - TAIL, 1) if place else tail
                tokens.append(jnp.concatenate([head, moved], axis=1)[:, :CHAN])
            lane = iota((1, 128), 1) - 2 * TAIL - 4
            flags = [
                jnp.sum(jnp.where(lane == i, tail[0:1], 0.0), axis=1, keepdims=True)
                for i in range(4)
            ]
            masks.append(region_mask(flags[0::2], flags[1::2]))
        x = jnp.concatenate(tokens, axis=0)
        mixed = attend(x, masks, bias_ref, gain_ref[...], wqv_ref, wk_ref)
        for index in range(pairs):
            rows = pl.ds(step * pairs + index, CHAN, stride=CAP)
            own = x[index * PAIR : (index + 1) * PAIR]
            done[rows, :] = own.T + dot(proj_ref[...], mixed[index])
        return carry

    lax.fori_loop(0, CAP // pairs, some_slots, 0)
    out_ref[...] = done[0 : CHAN * CAP, :].reshape(CHAN, CAP, PAIR).astype(BF16)


def work_path(got, bias, gain, wqv, wk, proj):
    return pl.pallas_call(
        work_kernel,
        in_specs=[VMEM] * 6,
        out_specs=VMEM,
        out_shape=jax.ShapeDtypeStruct((CHAN, CAP, PAIR), BF16),
        scratch_shapes=[
            pltpu.VMEM((TILE + 1, TOKENS * CAP, 128), F32),
            pltpu.VMEM((-(-CHAN // 8) * 8 * CAP, PAIR), F32),
        ],
        cost_estimate=pl.CostEstimate(
            flops=8_000_000_000, bytes_accessed=2_000_000, transcendentals=1_000_000
        ),
        name="work_path",
    )(in_vmem(got), in_vmem(bias), gain, in_vmem(wqv), in_vmem(wk), in_vmem(proj))


def from_behind(value, axis, steps):
    count = lax.axis_size(axis)
    pairs = [(source, (source + steps) % count) for source in range(count)]
    return lax.ppermute(value, axis, pairs)


def exchange(value):
    order = tuple((LEAD - j) % lax.axis_size("band") for j in range(lax.axis_size("band")))
    return lax.all_to_all(
        value, "band", split_axis=0, concat_axis=0, axis_index_groups=[order], tiled=True
    )


def shards(
    pixels,
    keep_mask,
    band_counts,
    plan_dest,
    plan_slot,
    bias_table,
    gain_attn,
    qkv_weight,
    proj_weight,
    gain_mlp,
    hidden_weight,
    output_weight,
):
    gain_attn, gain_mlp = gain_attn[None], gain_mlp[None]
    pixels = jnp.transpose(pixels, (2, 0, 1))
    outgoing, edge = spread(keep_mask, band_counts, plan_dest, plan_slot, pixels)
    halo = from_behind(in_vmem(edge), "band", 1)
    gathered = exchange(outgoing)
    sent, kept, wqv, wk, proj, bias = own_path(
        pixels,
        halo,
        bias_table.T,
        qkv_weight,
        proj_weight,
        gain_attn,
        gain_mlp,
        hidden_weight,
        output_weight.T,
    )
    lower = from_behind(sent, "band", -1)
    routed = route(gathered)
    incoming = exchange(routed)
    restored = jnp.concatenate([kept, lower], axis=1)
    restored = jnp.transpose(restored, (1, 2, 0))
    work_tiles = work_path(incoming, bias, gain_attn, wqv, wk, proj)
    work_tiles = jnp.transpose(work_tiles, (1, 2, 0))
    return (restored, work_tiles)


def solution(mesh):
    in_specs = (
        P(("img", "band"), None, None),
        P(("img", "band"), None),
        P(("img", "band")),
        P(("img", "band"), None),
        P(("img", "band"), None),
        P(),
        P(),
        P(),
        P(),
        P(),
        P(),
        P(),
    )
    out_specs = (P(("img", "band"), None, None), P(("img", "band"), None, None))
    return jax.shard_map(shards, mesh=mesh, in_specs=in_specs, out_specs=out_specs, check_vma=False)
```
